32 devices in a mesh: sta: 8 (over z, y), yr: 4 (over x, core).
Axes of the slice: x: 2, y: 2, z: 4, core: 2. Of those that a mesh axis runs over, the one named last changes fastest.
Arguments:
- temps: float32 [196608, 128], P(('sta', 'yr')), may hold values from -6 to 6
- day_bits: int32 [4, 196608], P(None, ('sta', 'yr')), may hold values from -2147483648 to 2147483646, as said below
- block_offset: int32 [196608], P(('sta', 'yr')), may hold values from 0 to 47
- block_counts: int32 [4, 2048], P('yr', 'sta'), may hold values from 0 to 48, as said below
- station_cell: int32 [2048], P('sta'), may hold values from 0 to 10367, as said below
Outputs:
- anomalies: float32 [196608, 128], P(('sta', 'yr'))
- climatology: float32 [10368, 384], P('sta')
The draws below stay inside these ranges and needn't reach their ends.
Inputs may be any that keep to these rules, and one draw needn't show every extreme that they name: `day_bits`: bit i of word w of a block's column says whether day 32 * w + i of the block was observed. `block_counts`: for each year range and station shard, the counts of the shard's 256 stations sum to 6144; in each of them some station has 48. `station_cell`: the owner of cell c is c // 1296. Of the 256 stations of one shard at most 128 lie in cells of one owner, and one owner has exactly 128 stations of every shard.
All inputs are finite; a program needn't handle non-finite values.
Results may differ from the reference program's by a relative error of at most 0.0003.
Values sent between devices are 32-bit elements; how exact they have to be, the bound alone decides.
A program may use at most 128 MiB of HBM per device.

```python
import jax
import jax.numpy as jnp
from jax import lax

DAYS = 128
CELLS = 10368
YR_DEV = 16
S_DEV = 256
MOST_BLOCKS = 48
BLK_DEV = 6144
STA_CAP = 128
STATIONS = 2048
BLOCKS = 196608


def draw_day_bits(key, part):
    return jax.random.randint(key, (DAYS // 32, BLOCKS), -2147483648, 2147483647, dtype=jnp.int32)


def draw_block_counts(key, part):
    shards = STATIONS // S_DEV
    groups = BLOCKS // BLK_DEV
    ranges = groups // shards
    half_most = MOST_BLOCKS // 2

    def group_counts(group_key):
        key_order, key_shift = jax.random.split(group_key)
        order_of = jax.random.permutation(key_order, S_DEV)
        shift_by = jax.random.randint(key_shift, (S_DEV // 2,), -half_most, half_most + 1, dtype=jnp.int32)
        shift_by = jnp.where(jnp.arange(S_DEV // 2, dtype=jnp.int32) == 0, half_most, shift_by)
        paired = jnp.concatenate([half_most + shift_by, half_most - shift_by]).astype(jnp.int32)
        return jnp.zeros((S_DEV,), jnp.int32).at[order_of].set(paired)
    counts = jax.vmap(group_counts)(jax.random.split(key, groups))
    return counts.reshape(ranges, shards * S_DEV).astype(jnp.int32)


def draw_station_cell(key, part):
    shards = STATIONS // S_DEV
    capacity = STA_CAP
    cell_dev = CELLS // shards
    key_hot, key_rest = jax.random.split(key)
    hot_owner = jax.random.randint(key_hot, (), 0, shards, dtype=jnp.int32)

    def shard_cells(shard_key):
        key_order, key_others, key_cell = jax.random.split(shard_key, 3)
        order_of = jax.random.permutation(key_order, S_DEV)
        others = (hot_owner + 1 + jax.random.permutation(key_others, shards - 1).astype(jnp.int32)) % shards
        slot_rank = jnp.arange(S_DEV, dtype=jnp.int32)
        group_of = jnp.clip((slot_rank - capacity) // (capacity // 2), 0, shards - 2)
        owner_ranked = jnp.where(slot_rank < capacity, hot_owner, others[group_of]).astype(jnp.int32)
        owner_of = jnp.zeros((S_DEV,), jnp.int32).at[order_of].set(owner_ranked)
        local_cell = jax.random.randint(key_cell, (S_DEV,), 0, cell_dev, dtype=jnp.int32)
        return owner_of * cell_dev + local_cell
    cells = jax.vmap(shard_cells)(jax.random.split(key_rest, shards))
    return cells.reshape(-1).astype(jnp.int32)


def set_ends(array, stream_key, least, top_value):
    place = [jax.random.randint(jax.random.fold_in(stream_key, axis), (), 0, length) for axis, length in enumerate(array.shape)]
    main_axis = array.shape.index(max(array.shape))
    next_to = place[:main_axis] + [(place[main_axis] + 1) % array.shape[main_axis]] + place[main_axis + 1:]
    return array.at[tuple(place)].set(least).at[tuple(next_to)].set(top_value)


def shard_levels(key, dims, cuts, least, high):
    level, own = 1.0, jax.random.fold_in(key, 6)
    for dim, shards_of in cuts:
        steps = jnp.exp(jax.random.uniform(jax.random.fold_in(own, dim), (shards_of,), jnp.float32, least / len(cuts), high / len(cuts)))
        level = level * jnp.repeat(steps, dims[dim] // shards_of).reshape([-1 if axis == dim else 1 for axis in range(len(dims))])
    return level


def gaussian(own_key, shape, spread, bound, cuts=(), kind=jnp.bfloat16):
    array = jax.random.normal(own_key, shape, jnp.float32) * spread
    if len(cuts) > 0:
        array = shard_levels(own_key, shape, cuts, -0.22, 0.18) * array
    return jnp.clip(array, min=-bound, max=bound).astype(kind)


def setup_inputs(seed: int = 0) -> dict:
    key_of = jax.random.split(jax.random.key(seed), 6)
    return {
        "temps": gaussian(key_of[0], (BLOCKS, DAYS), 1.0, 6.0, ((0, 32),), jnp.float32),
        "day_bits": draw_day_bits(jax.random.fold_in(key_of[5], 71), 0),
        "block_offset": set_ends(jax.random.randint(key_of[2], (BLOCKS,), 0, 3 * YR_DEV), jax.random.fold_in(key_of[2], 1), 0, (3 * YR_DEV) - 1).astype(jnp.int32),
        "block_counts": draw_block_counts(jax.random.fold_in(key_of[5], 71), 0),
        "station_cell": draw_station_cell(jax.random.fold_in(key_of[5], 71), 0),
    }


CALENDAR = 365


def observed_days(packed, offsets):
    day_count = packed.shape[0] * 32
    shifts = jnp.arange(32, dtype=jnp.int32)
    bit_values = jnp.right_shift(packed[:, None, :], shifts[None, :, None]) & 1
    bit_values = bit_values.reshape(day_count, packed.shape[1]).T
    thirds = (offsets % 3).astype(jnp.int32)
    season_day = thirds[:, None] * day_count + jnp.arange(day_count, dtype=jnp.int32)[None, :]
    observed = jnp.where((bit_values == 1) & (season_day < CALENDAR), 1.0, 0.0).astype(jnp.float32)
    return observed, thirds


def slot_stations(counts, block_total):
    ends_at = jnp.cumsum(counts).astype(jnp.int32)
    slot_ids = jnp.arange(block_total, dtype=jnp.int32)
    return jnp.searchsorted(ends_at, slot_ids, side="right").astype(jnp.int32)


def reference(temps, day_bits, block_offset, block_counts, station_cell):
    shards = STATIONS // S_DEV
    ranges = block_counts.shape[0]
    groups = shards * ranges
    row_width = 3 * DAYS
    temps_grouped = temps.reshape(groups, BLK_DEV, DAYS)
    packed_grouped = jnp.transpose(day_bits.reshape(DAYS // 32, groups, BLK_DEV), (1, 0, 2))
    offsets_grouped = block_offset.reshape(groups, BLK_DEV)
    counts_grouped = jnp.transpose(block_counts.reshape(ranges, shards, S_DEV), (1, 0, 2)).reshape(groups, S_DEV)

    def first_pass(inputs):
        values, packed, offsets, counts = inputs
        observed, thirds = observed_days(packed, offsets)
        segment = slot_stations(counts, BLK_DEV) * 3 + thirds
        total_sums = jax.ops.segment_sum(observed * values, segment, num_segments=S_DEV * 3)
        tallies = jax.ops.segment_sum(observed, segment, num_segments=S_DEV * 3)
        return total_sums.reshape(S_DEV, row_width), tallies.reshape(S_DEV, row_width)

    station_sums, station_tallies = lax.map(first_pass, (temps_grouped, packed_grouped, offsets_grouped, counts_grouped))
    station_sums = jnp.sum(station_sums.reshape(shards, ranges, S_DEV, row_width), axis=1).reshape(STATIONS, row_width)
    station_tallies = jnp.sum(station_tallies.reshape(shards, ranges, S_DEV, row_width), axis=1).reshape(STATIONS, row_width)
    cell_sums = jax.ops.segment_sum(station_sums, station_cell, num_segments=CELLS)
    cell_tallies = jax.ops.segment_sum(station_tallies, station_cell, num_segments=CELLS)
    climatology = cell_sums / jnp.maximum(cell_tallies, 1.0)
    station_clim = climatology[station_cell].reshape(shards, S_DEV * 3, DAYS)

    def second_pass(inputs):
        group_index, values, packed, offsets, counts = inputs
        observed, thirds = observed_days(packed, offsets)
        segment = slot_stations(counts, BLK_DEV) * 3 + thirds
        shard_clim = lax.dynamic_index_in_dim(station_clim, group_index // ranges, 0, keepdims=False)
        block_clim = shard_clim[segment]
        return observed * (values - block_clim)

    anomalies = lax.map(second_pass, (jnp.arange(groups, dtype=jnp.int32), temps_grouped, packed_grouped, offsets_grouped, counts_grouped))
    return anomalies.reshape(BLOCKS, DAYS), climatology
```

```python
import functools

import jax
import jax.numpy as jnp
from jax import lax
from jax.experimental import pallas as pl
from jax.experimental.pallas import tpu as pltpu
from jax.sharding import PartitionSpec as P

CELLS = 10368
CALENDAR = 365
MOST_BLOCKS = 48
LANES = 128
TILE = 8
F32 = jnp.float32
BF16 = jnp.bfloat16
I32 = jnp.int32
VMEM = pltpu.VMEM


def round_up(value, step):
    return (value + step - 1) // step * step


def tally_words(ranges):
    if ranges * MOST_BLOCKS < 256:
        return [(0, 1, 2)], 256
    return [(0, 1), (2,)], 4096


def iota(shape, dim):
    return lax.broadcasted_iota(I32, shape, dim)


def one_where(mask):
    return jnp.where(mask, 1.0, 0.0).astype(BF16)


def dot(a, b, dims=((1,), (0,))):
    return lax.dot_general(a, b, (dims, ((), ())), preferred_element_type=F32)


def split_two(value):
    high = value.astype(BF16)
    return high, (value - high.astype(F32)).astype(BF16)


def row_stations(counts, blocks):
    stations = counts.shape[1]
    spread = jnp.broadcast_to(counts.astype(F32), (LANES, stations)).astype(BF16)
    square = (stations, stations)
    ends = dot(one_where(iota(square, 1) <= iota(square, 0)), spread, ((1,), (1,))).astype(I32)
    lane = iota((stations, LANES), 1)
    ending = dot(one_where((ends >> 7) == lane), one_where((ends & 127) == lane), ((0,), (0,)))
    ending = ending.astype(BF16)
    tile = (LANES, LANES)
    within = dot(ending, one_where(iota(tile, 0) <= iota(tile, 1)))
    totals = dot(ending, jnp.ones(tile, BF16)).astype(BF16)
    before = dot(one_where(iota(tile, 1) < iota(tile, 0)), totals)
    return (within + before)[:blocks]


def sums_kernel(
    ranges, rows, temps_hbm, bits_hbm, offs_hbm, counts_hbm, cell_hbm,
    sums_ref, masked_ref, code_ref, cells_ref, bits, offs, counts, acc, tally, small, large,
):
    block_total = masked_ref.shape[0]
    blocks, stations = offs.shape[0], counts.shape[1]
    words, base = tally_words(ranges)
    chunk_count = sums_ref.shape[1]
    firsts = [
        pltpu.make_async_copy(counts_hbm, counts, small.at[0]),
        pltpu.make_async_copy(offs_hbm, offs, small.at[1]),
        pltpu.make_async_copy(bits_hbm, bits, small.at[2]),
        pltpu.make_async_copy(cell_hbm, cells_ref.at[0 : cell_hbm.shape[0]], small.at[3]),
    ]
    steps = block_total // rows
    loads = [
        pltpu.make_async_copy(
            temps_hbm.at[i * rows : (i + 1) * rows], masked_ref.at[i * rows : (i + 1) * rows],
            large.at[i],
        )
        for i in range(steps)
    ]
    for copy in firsts + loads:
        copy.start()
    firsts[0].wait()
    station = row_stations(counts[...], blocks)
    firsts[1].wait()
    offsets = offs[...]
    third = offsets - 3 * ((offsets * 21846) >> 16)
    double_segment = 2 * (third * stations + station.astype(I32))
    limit = CALENDAR - LANES * third
    station_of = [jnp.where(third == k, station, -1.0).astype(BF16) for k in range(3)]
    weight_of = []
    for held in words:
        weight = jnp.zeros(third.shape, F32)
        for place, k in enumerate(held):
            weight = jnp.where(third == k, float(base**place), weight)
        weight_of.append(weight.astype(BF16))
    station = station.astype(BF16)
    at = iota((stations, LANES), 0).astype(F32).astype(BF16)
    day = iota((LANES, LANES), 0)
    shift = day & 31
    one, zero = jnp.ones((), BF16), jnp.zeros((), BF16)
    firsts[2].wait()
    for i in range(steps):
        loads[i].wait()
        values, observed_all, hots, weights = [], [], [], []
        for q in range(i * rows // LANES, (i + 1) * rows // LANES):
            here = slice(q * LANES, (q + 1) * LANES)
            packed = jnp.concatenate(
                [jnp.broadcast_to(bits[w : w + 1, here], (32, LANES)) for w in range(bits.shape[0])],
                axis=0,
            )
            bit = (packed >> shift) & 1
            code = jnp.where(day < limit[q : q + 1], bit, 0) + double_segment[q : q + 1]
            code = code.T
            code_ref[here] = code
            observed = (code & 1).astype(F32)
            value = masked_ref[here] * observed
            masked_ref[here] = value
            values.append(jnp.concatenate(split_two(value), axis=1))
            observed_all.append(observed.astype(BF16))
            hots.append(
                jnp.concatenate(
                    [
                        jnp.where(at == jnp.broadcast_to(s[q : q + 1], at.shape), one, zero)
                        for s in station_of
                    ],
                    axis=0,
                )
            )
            inside = at == jnp.broadcast_to(station[q : q + 1], at.shape)
            weights.append(
                jnp.concatenate(
                    [
                        jnp.where(inside, jnp.broadcast_to(w[q : q + 1], at.shape), zero)
                        for w in weight_of
                    ],
                    axis=0,
                )
            )
        total = dot(jnp.concatenate(hots, axis=1), jnp.concatenate(values, axis=0))
        count = dot(jnp.concatenate(weights, axis=1), jnp.concatenate(observed_all, axis=0))
        acc[...] = total if i == 0 else acc[...] + total
        tally[...] = count if i == 0 else tally[...] + count
    split = (ranges, chunk_count, TILE, stations)
    for k in range(3):
        part = acc[k * stations : (k + 1) * stations]
        sums_ref[:, :, k] = (part[:, :LANES] + part[:, LANES:]).T.reshape(split)
    for w in range(len(words)):
        sums_ref[:, :, 3 + w] = tally[w * stations : (w + 1) * stations].T.reshape(split)
    firsts[3].wait()


def remote(src, dst, send, recv, where):
    return pltpu.make_async_remote_copy(
        src_ref=src, dst_ref=dst, send_sem=send, recv_sem=recv,
        device_id=where, device_id_type=pl.DeviceIdType.MESH,
    )


def greet(peers):
    barrier = pltpu.get_barrier_semaphore()
    for where in peers:
        pl.semaphore_signal(barrier, inc=1, device_id=where, device_id_type=pl.DeviceIdType.MESH)
    pl.semaphore_wait(barrier, len(peers))


def pick(index, table):
    value = jnp.int32(table[0])
    for i in range(1, len(table)):
        value = jnp.where(index == i, jnp.int32(table[i]), value)
    return value


def exchange_kernel(
    ranges, owners, major, cell_dev, cell_pad, sums_ref, cells_ref, out_ref,
    ids, pair, partial, across, got, lhs, hot,
    id_send, id_recv, pair_send, pair_recv, across_send, across_recv,
    col_send, col_recv, row_send, row_recv, far_send, far_recv, near_send, near_recv,
):
    _, chunks, groups, _, stations = sums_ref.shape
    halves = stations // LANES
    words, base = tally_words(ranges)
    width = out_ref.shape[-1]
    chips, minor = ranges // 2, owners // major
    sta, yr = lax.axis_index("sta"), lax.axis_index("yr")
    chip, core = yr // 2, lax.rem(yr, 2)
    row, place = sta // minor, lax.rem(sta, minor)
    partner = {"yr": chip * 2 + 1 - core}
    chip_at = [lax.rem(chip + k, chips) for k in range(chips)]
    chip_from = [lax.rem(chip + chips - k, chips) for k in range(chips)]
    near_first = [
        sorted((r for r in range(major) if r != mine), key=lambda r: (abs(r - mine), r))
        for mine in range(major)
    ]
    rows_by = [pick(row, [near_first[m][i] for m in range(major)]) for i in range(major - 1)]

    greet(
        [partner]
        + [{"yr": c * 2 + core} for c in chip_at[1:]]
        + [{"sta": lax.rem(sta + j, owners)} for j in range(1, owners)]
    )
    id_copies = []
    for j in range(1, owners):
        copy = remote(
            cells_ref, ids.at[sta], id_send.at[j - 1], id_recv.at[j - 1],
            {"sta": lax.rem(sta + j, owners)},
        )
        copy.start()
        id_copies.append(copy)
    pairs = []
    for c in range(chunks):
        for k in [*range(1, chips), 0]:
            copy = remote(
                sums_ref.at[chip_at[k] * 2 + 1 - core, c], pair.at[c, k],
                pair_send.at[c, k], pair_recv.at[c, k], partner,
            )
            copy.start()
            pairs.append(copy)
    ids[sta] = cells_ref[...]
    crossing = []
    for c in range(chunks):
        for k in range(1, chips):
            pairs[c * chips + k - 1].wait_recv()
            partial[c, k - 1] = sums_ref[chip_at[k] * 2 + core, c] + pair[c, k]
            copy = remote(
                partial.at[c, k - 1], across.at[c, k - 1],
                across_send.at[c, k - 1], across_recv.at[c, k - 1],
                {"yr": chip_at[k] * 2 + core},
            )
            copy.start()
            crossing.append(copy)

    def col(c, i):
        block = got.at[c, sta]
        return remote(
            block, block, col_send.at[c, i], col_recv.at[c, row],
            {"sta": rows_by[i] * minor + place},
        )

    def col_in(c, i):
        block = got.at[c, rows_by[i] * minor + place]
        return remote(
            block, block, col_send.at[c, i], col_recv.at[c, rows_by[i]],
            {"sta": rows_by[i] * minor + place},
        )

    def across_row(c, from_row, j):
        block = got.at[c, from_row * minor + place]
        return remote(
            block, block, row_send.at[c, from_row, j - 1], row_recv.at[c, from_row, j - 1],
            {"sta": row * minor + lax.rem(place + j, minor)},
        )

    def row_in(c, from_row, j):
        block = got.at[c, from_row * minor + lax.rem(place + minor - j, minor)]
        return remote(
            block, block, row_send.at[c, from_row, j - 1], row_recv.at[c, from_row, j - 1],
            {"sta": row * minor + lax.rem(place + minor - j, minor)},
        )

    def own(c):
        pairs[c * chips + chips - 1].wait_recv()
        total = sums_ref[yr, c] + pair[c, 0]
        for k in range(chips - 1):
            crossing[c * (chips - 1) + k].wait_recv()
            total = total + across[c, k]
        got[c, sta] = total
        for i in range(major - 1):
            col(c, i).start()
        for j in range(1, minor):
            across_row(c, row, j).start()

    def forward(c, then=lambda i: None):
        for i in range(major - 1):
            then(i)
            col_in(c, i).wait_recv()
            for j in range(1, minor):
                across_row(c, rows_by[i], j).start()
        then(major - 1)

    lane = iota((1, width), 1)
    mine = jnp.concatenate(
        [jnp.full((1, cell_pad), -1, I32)] + [cells_ref[h : h + 1] for h in range(halves)], axis=1
    )
    target = jnp.where(lane < cell_dev, lane + sta * cell_dev, mine)

    def build(first, last):
        for s in range(first, last):
            column = ids[s].T
            for h in range(halves):
                at = s * stations + h * LANES
                hot[at : at + LANES] = one_where(column[:, h : h + 1] == target)

    def cells(c):
        for j in range(1, minor):
            row_in(c, row, j).wait_recv()
            for i in range(major - 1):
                row_in(c, rows_by[i], j).wait_recv()
        for s in range(owners):
            sums = [got[c, s, k] for k in range(3)]
            high = [v.astype(BF16).astype(F32) for v in sums]
            low = [v - h for v, h in zip(sums, high)]
            tallies = [None] * 3
            for w, held in enumerate(words):
                word = got[c, s, 3 + w].astype(I32)
                for p, k in enumerate(held):
                    tallies[k] = ((word // base**p) & (base - 1)).astype(F32)
            parts = high + low + tallies
            if base > 256:
                rounded = [t.astype(BF16).astype(F32) for t in tallies]
                parts = high + low + rounded + [t - r for t, r in zip(tallies, rounded)]
            if len(parts) % 2:
                parts.append(jnp.zeros_like(parts[0]))
            lhs[:, s * stations : (s + 1) * stations] = jnp.concatenate(parts, axis=0).astype(BF16)
        total = dot(lhs[...], hot[...])
        step = 3 * TILE
        tally = total[2 * step : 3 * step]
        if base > 256:
            tally = tally + total[3 * step : 4 * step]
        clim = (total[:step] + total[step : 2 * step]) / jnp.maximum(tally, 1.0)
        out_ref[yr, c] = clim.reshape(3, TILE, width)
        block = out_ref.at[yr, c]
        for k in range(1, chips):
            far(c, k).start()
        near(c, 0).start()

    def far(c, k):
        block = out_ref.at[yr, c]
        return remote(
            block, block, far_send.at[c, k - 1], far_recv.at[c, k - 1],
            {"yr": chip_at[k] * 2 + core},
        )

    def near(c, k):
        block = out_ref.at[chip_from[k] * 2 + core, c]
        return remote(block, block, near_send.at[c, k], near_recv.at[c, k], partner)

    def hand_on(c):
        for k in range(1, chips):
            far(c, k).wait_recv()
            near(c, k).start()

    for c in range(chunks):
        own(c)
    for copy in id_copies:
        copy.wait_recv()
    share = -(-owners // major)
    forward(0, lambda i: build(i * share, min((i + 1) * share, owners)))
    for c in range(chunks):
        if c + 1 < chunks:
            forward(c + 1)
        cells(c)
        if c >= 2:
            hand_on(c - 2)
    for c in range(max(chunks - 2, 0), chunks):
        hand_on(c)
    for c in range(chunks):
        for k in range(chips):
            near(c, k).wait()
        for k in range(1, chips):
            far(c, k).wait_send()
        for i in range(major - 1):
            col(c, i).wait_send()
        for j in range(1, minor):
            across_row(c, row, j).wait_send()
            for i in range(major - 1):
                across_row(c, rows_by[i], j).wait_send()
    for copy in id_copies + pairs + crossing:
        copy.wait_send()


def anomaly_kernel(
    ranges, cell_dev, cell_pad, rows, masked_ref, code_ref, clim_ref,
    out_hbm, climatology_hbm, table, clim_buf, out_buf, clim_sem, out_sem,
):
    block_total, days = masked_ref.shape
    stations = clim_ref.shape[-1] - cell_pad
    for k in range(3):
        part = clim_ref[:, :, k, :, cell_pad:].reshape(days, stations)
        high, low = split_two(part)
        table[:days, k * stations : (k + 1) * stations] = high
        table[days:, k * stations : (k + 1) * stations] = low
    for j in range(cell_pad // LANES):
        for k in range(3):
            part = clim_ref[:, :, k, :, j * LANES : (j + 1) * LANES].reshape(days, LANES)
            last = min((j + 1) * LANES, cell_dev)
            clim_buf[j * LANES : last, k * days : (k + 1) * days] = part.T[: last - j * LANES]
    clim_copy = pltpu.make_async_copy(clim_buf, climatology_hbm, clim_sem.at[0])
    clim_copy.start()
    copies = []
    for i in range(block_total // rows):
        here = slice(i * rows, (i + 1) * rows)
        code = code_ref[here]
        segment = code >> 1
        lane = iota(code.shape, 1)
        hot = jnp.concatenate(
            [one_where(segment == lane + j * LANES) for j in range(3 * stations // LANES)], axis=1
        )
        found = dot(hot, table[...], ((1,), (1,)))
        clim = found[:, :days] + found[:, days:]
        out_buf[here] = masked_ref[here] - (code & 1).astype(F32) * clim
        copy = pltpu.make_async_copy(out_buf.at[here], out_hbm.at[here], out_sem.at[i])
        copy.start()
        copies.append(copy)
    for copy in [clim_copy] + copies:
        copy.wait()


def per_device(temps, day_bits, block_offset, block_counts, station_cell):
    owners, ranges = lax.axis_size("sta"), lax.axis_size("yr")
    stations = station_cell.shape[0]
    block_total, days = temps.shape
    cell_dev = CELLS // owners
    cell_pad = round_up(cell_dev, LANES)
    width = cell_pad + stations
    words, base = tally_words(ranges)
    groups = 3 + len(words)
    chunks = days // ranges // TILE
    rows = 1024 if block_total % 1024 == 0 else block_total
    major = 4 if owners % 4 == 0 else owners
    minor, chips = owners // major, ranges // 2
    dma = pltpu.SemaphoreType.DMA
    whole = pl.BlockSpec(memory_space=VMEM)
    hbm = pl.BlockSpec(memory_space=pltpu.HBM)

    inputs = [
        pltpu.with_memory_space_constraint(array, pltpu.HBM)
        for array in (
            temps, day_bits, block_offset.reshape(block_total // LANES, LANES), block_counts,
            station_cell.reshape(stations // LANES, LANES),
        )
    ]
    sums, masked, code, cells = pl.pallas_call(
        functools.partial(sums_kernel, ranges, rows),
        in_specs=[hbm] * 5,
        out_specs=[whole] * 4,
        out_shape=[
            jax.ShapeDtypeStruct((ranges, chunks, groups, TILE, stations), F32),
            jax.ShapeDtypeStruct((block_total, days), F32),
            jax.ShapeDtypeStruct((block_total, days), I32),
            jax.ShapeDtypeStruct((TILE, LANES), I32),
        ],
        scratch_shapes=[
            VMEM((day_bits.shape[0], block_total), I32),
            VMEM((block_total // LANES, LANES), I32),
            VMEM((1, stations), I32),
            VMEM((3 * stations, 2 * days), F32),
            VMEM((len(words) * stations, days), F32),
            dma((4,)), dma((block_total // rows,)),
        ],
        compiler_params=pltpu.CompilerParams(vmem_limit_bytes=40 * 1024 * 1024),
    )(*inputs)

    block = (groups, TILE, stations)
    parts = 3 * 3 if base <= 256 else 3 * 4
    crossings, others, sides = max(chips - 1, 1), max(major - 1, 1), max(minor - 1, 1)
    clim = pl.pallas_call(
        functools.partial(exchange_kernel, ranges, owners, major, cell_dev, cell_pad),
        in_specs=[whole] * 2,
        out_specs=whole,
        out_shape=jax.ShapeDtypeStruct((ranges, chunks, 3, TILE, width), F32),
        scratch_shapes=[
            VMEM((owners, TILE, LANES), I32),
            VMEM((chunks, chips) + block, F32),
            VMEM((chunks, crossings) + block, F32),
            VMEM((chunks, crossings) + block, F32),
            VMEM((chunks, owners) + block, F32),
            VMEM((round_up(parts * TILE, 16), owners * stations), BF16),
            VMEM((owners * stations, width), BF16),
            dma((owners - 1,)), dma((owners - 1,)),
            dma((chunks, chips)), dma((chunks, chips)),
            dma((chunks, crossings)), dma((chunks, crossings)),
            dma((chunks, others)), dma((chunks, major)),
            dma((chunks, major, sides)), dma((chunks, major, sides)),
            dma((chunks, crossings)), dma((chunks, crossings)),
            dma((chunks, chips)), dma((chunks, chips)),
        ],
        compiler_params=pltpu.CompilerParams(
            collective_id=0, has_side_effects=True, vmem_limit_bytes=40 * 1024 * 1024
        ),
    )(sums, cells)

    rows = 512 if block_total % 512 == 0 else block_total
    return pl.pallas_call(
        functools.partial(anomaly_kernel, ranges, cell_dev, cell_pad, rows),
        in_specs=[whole] * 3,
        out_specs=[hbm] * 2,
        out_shape=[
            jax.ShapeDtypeStruct((block_total, days), F32),
            jax.ShapeDtypeStruct((cell_dev, 3 * days), F32),
        ],
        scratch_shapes=[
            VMEM((2 * days, 3 * stations), BF16),
            VMEM((cell_dev, 3 * days), F32),
            VMEM((block_total, days), F32),
            dma((1,)), dma((block_total // rows,)),
        ],
        compiler_params=pltpu.CompilerParams(vmem_limit_bytes=40 * 1024 * 1024),
    )(masked, code, clim)


def solution(mesh):
    in_specs = (
        P(("sta", "yr"), None),
        P(None, ("sta", "yr")),
        P(("sta", "yr")),
        P("yr", "sta"),
        P("sta"),
    )
    out_specs = (P(("sta", "yr"), None), P("sta", None))

    def run(*args):
        return tuple(per_device(*args))

    return jax.shard_map(
        run, mesh=mesh, in_specs=in_specs, out_specs=out_specs, check_vma=False
    )
```

```python
import functools

import jax
import jax.numpy as jnp
from jax import lax
from jax.experimental import pallas as pl
from jax.experimental.pallas import tpu as pltpu
from jax.sharding import PartitionSpec as P

CELLS = 10368
CALENDAR = 365
MOST_BLOCKS = 48
LANES = 128
TILE = 8
GROUP = 16
WINDOW = 256
NEARBY = 96
F32 = jnp.float32
BF16 = jnp.bfloat16
I32 = jnp.int32
VMEM = pltpu.VMEM


def round_up(value, step):
    return (value + step - 1) // step * step


def tally_words(ranges):
    if ranges * MOST_BLOCKS < 256:
        return [(0, 1, 2)], 256
    return [(0, 1), (2,)], 4096


def iota(shape, dim):
    return lax.broadcasted_iota(I32, shape, dim)


def one_where(mask):
    return jnp.where(mask, 1.0, 0.0).astype(BF16)


def dot(a, b, dims=((1,), (0,))):
    return lax.dot_general(a, b, (dims, ((), ())), preferred_element_type=F32)


def split_two(value):
    high = value.astype(BF16)
    return high, (value - high.astype(F32)).astype(BF16)


def row_stations(counts, blocks):
    stations = counts.shape[1]
    spread = jnp.broadcast_to(counts.astype(F32), (LANES, stations)).astype(BF16)
    square = (stations, stations)
    ends = dot(one_where(iota(square, 1) <= iota(square, 0)), spread, ((1,), (1,))).astype(I32)
    lane = iota((stations, LANES), 1)
    ending = dot(one_where((ends >> 7) == lane), one_where((ends & 127) == lane), ((0,), (0,)))
    ending = ending.astype(BF16)
    tile = (LANES, LANES)
    within = dot(ending, one_where(iota(tile, 0) <= iota(tile, 1)))
    totals = dot(ending, jnp.ones(tile, BF16)).astype(BF16)
    before = dot(one_where(iota(tile, 1) < iota(tile, 0)), totals)
    return (within + before)[:blocks]


def sums_kernel(
    ranges, rows, temps_hbm, bits_hbm, offs_hbm, counts_hbm, cell_hbm,
    sums_ref, masked_ref, code_ref, cells_ref, bits, offs, counts, acc, tally, small, large,
):
    block_total = masked_ref.shape[0]
    blocks, stations = offs.shape[0], counts.shape[1]
    words, base = tally_words(ranges)
    chunk_count = sums_ref.shape[1]
    firsts = [
        pltpu.make_async_copy(counts_hbm, counts, small.at[0]),
        pltpu.make_async_copy(offs_hbm, offs, small.at[1]),
        pltpu.make_async_copy(bits_hbm, bits, small.at[2]),
        pltpu.make_async_copy(cell_hbm, cells_ref.at[0 : cell_hbm.shape[0]], small.at[3]),
    ]
    steps = block_total // rows
    loads = [
        pltpu.make_async_copy(
            temps_hbm.at[i * rows : (i + 1) * rows], masked_ref.at[i * rows : (i + 1) * rows],
            large.at[i],
        )
        for i in range(steps)
    ]
    for copy in firsts + loads:
        copy.start()
    firsts[0].wait()
    station = row_stations(counts[...], blocks)
    firsts[1].wait()
    offsets = offs[...]
    third = offsets - 3 * ((offsets * 21846) >> 16)
    station = station.astype(I32)
    segment = (station // GROUP) * (3 * GROUP) + third * GROUP + station % GROUP
    double_segment = 2 * segment
    limit = CALENDAR - LANES * third
    weight_of = []
    for held in words:
        weight = jnp.zeros(third.shape, F32)
        for place, k in enumerate(held):
            weight = jnp.where(third == k, float(base**place), weight)
        weight_of.append(weight.astype(BF16))
    group = station // GROUP
    per_step = rows // LANES
    low = [jnp.min(group[i * per_step : (i + 1) * per_step]) for i in range(steps)]
    high = [jnp.max(group[i * per_step : (i + 1) * per_step]) for i in range(steps)]
    close = functools.reduce(jnp.logical_and, [h - l < WINDOW // (3 * GROUP) for l, h in zip(low, high)])
    at = iota((WINDOW, LANES), 0).astype(F32).astype(BF16)
    day = iota((LANES, LANES), 0)
    shift = day & 31
    one, zero = jnp.ones((), BF16), jnp.zeros((), BF16)
    acc[...] = jnp.zeros_like(acc)
    tally[...] = jnp.zeros_like(tally)
    firsts[2].wait()
    for q in range(blocks):
        here = slice(q * LANES, (q + 1) * LANES)
        packed = jnp.concatenate(
            [jnp.broadcast_to(bits[w : w + 1, here], (32, LANES)) for w in range(bits.shape[0])],
            axis=0,
        )
        bit = (packed >> shift) & 1
        code = jnp.where(day < limit[q : q + 1], bit, 0) + double_segment[q : q + 1]
        code_ref[here] = code.T
    for copy in loads:
        copy.wait()

    def against(number, start, size):
        return jnp.clip(number - start, -1, size).astype(F32).astype(BF16)

    def spread(lines, q, size):
        return jnp.broadcast_to(lines[q : q + 1], (size, LANES))

    def add_up(windows_of, nearby_of):
        for i in range(steps):
            values, observed_all = [], []
            blocks_here = range(i * per_step, (i + 1) * per_step)
            for q in blocks_here:
                here = slice(q * LANES, (q + 1) * LANES)
                observed = (code_ref[here] & 1).astype(F32)
                value = masked_ref[here] * observed
                masked_ref[here] = value
                values.append(jnp.concatenate(split_two(value), axis=1))
                observed_all.append(observed.astype(BF16))
            values = jnp.concatenate(values, axis=0)
            observed_all = jnp.concatenate(observed_all, axis=0)
            for start in windows_of(i):
                place = against(segment, start, WINDOW)
                hot = jnp.concatenate(
                    [jnp.where(at == spread(place, q, WINDOW), one, zero) for q in blocks_here], axis=1
                )
                acc[pl.ds(start, WINDOW)] += dot(hot, values)
            for start in nearby_of(i):
                place = against(station, start, NEARBY)
                for w, weight in enumerate(weight_of):
                    hot = jnp.concatenate(
                        [
                            jnp.where(
                                at[:NEARBY] == spread(place, q, NEARBY), spread(weight, q, NEARBY), zero
                            )
                            for q in blocks_here
                        ],
                        axis=1,
                    )
                    tally[w, pl.ds(start, NEARBY)] += dot(hot, observed_all)

    @pl.when(close)
    def _():
        add_up(
            lambda i: [pl.multiple_of(low[i] * (3 * GROUP), GROUP)],
            lambda i: [pl.multiple_of(low[i] * GROUP, GROUP)],
        )

    @pl.when(jnp.logical_not(close))
    def _():
        add_up(
            lambda i: range(0, 3 * stations, WINDOW), lambda i: range(0, stations, NEARBY)
        )

    split = (ranges, chunk_count, TILE, stations)
    for k in range(3):
        part = jnp.concatenate(
            [
                acc[(3 * g + k) * GROUP : (3 * g + k + 1) * GROUP]
                for g in range(stations // GROUP)
            ],
            axis=0,
        )
        sums_ref[:, :, k] = (part[:, :LANES] + part[:, LANES:]).T.reshape(split)
    for w in range(len(words)):
        sums_ref[:, :, 3 + w] = tally[w, :stations].T.reshape(split)
    firsts[3].wait()


def remote(src, dst, send, recv, where):
    return pltpu.make_async_remote_copy(
        src_ref=src, dst_ref=dst, send_sem=send, recv_sem=recv,
        device_id=where, device_id_type=pl.DeviceIdType.MESH,
    )


def greet(peers):
    barrier = pltpu.get_barrier_semaphore()
    for where in peers:
        pl.semaphore_signal(barrier, inc=1, device_id=where, device_id_type=pl.DeviceIdType.MESH)
    pl.semaphore_wait(barrier, len(peers))


def pick(index, table):
    value = jnp.int32(table[0])
    for i in range(1, len(table)):
        value = jnp.where(index == i, jnp.int32(table[i]), value)
    return value


def exchange_kernel(
    ranges, owners, major, cap, cell_dev, cell_pad, sums_ref, cells_ref, out_ref,
    ids, pair, partial, across, got, lhs, hot, clim_ref, unpack,
    id_send, id_recv, pair_send, pair_recv, across_send, across_recv,
    col_send, col_recv, row_send, row_recv, far_send, far_recv, near_send, near_recv,
):
    _, chunks, groups, _, stations = sums_ref.shape
    halves = stations // LANES
    words, base = tally_words(ranges)
    width = clim_ref.shape[-1]
    slots = width - stations
    chips, minor = ranges // 2, owners // major
    sta, yr = lax.axis_index("sta"), lax.axis_index("yr")
    chip, core = yr // 2, lax.rem(yr, 2)
    row, place = sta // minor, lax.rem(sta, minor)
    partner = {"yr": chip * 2 + 1 - core}
    chip_at = [lax.rem(chip + k, chips) for k in range(chips)]
    chip_from = [lax.rem(chip + chips - k, chips) for k in range(chips)]
    near_first = [
        sorted(
            (r for r in range(major) if r != mine),
            key=lambda r: (abs(r - mine), r if 2 * mine < major else -r),
        )
        for mine in range(major)
    ]
    relayed = major == 4
    inner = (row == 1) | (row == 2)
    turned = [relayed and c % 2 == 1 for c in range(chunks)]
    rows_by = [pick(row, [near_first[m][i] for m in range(major)]) for i in range(major - 1)]

    greet(
        [partner]
        + [{"yr": c * 2 + core} for c in chip_at[1:]]
        + [{"sta": lax.rem(sta + j, owners)} for j in range(1, owners)]
    )
    id_copies = []
    for j in range(1, owners):
        copy = remote(
            cells_ref, ids.at[sta], id_send.at[j - 1], id_recv.at[j - 1],
            {"sta": lax.rem(sta + j, owners)},
        )
        copy.start()
        id_copies.append(copy)
    pairs = []
    for c in range(chunks):
        for k in [*range(1, chips), 0]:
            copy = remote(
                sums_ref.at[chip_at[k] * 2 + 1 - core, c], pair.at[c, k],
                pair_send.at[c, k], pair_recv.at[c, k], partner,
            )
            copy.start()
            pairs.append(copy)
    ids[sta] = cells_ref[...]
    crossing = []
    for c in range(chunks):
        for k in range(1, chips):
            pairs[c * chips + k - 1].wait_recv()
            partial[c, k - 1] = sums_ref[chip_at[k] * 2 + core, c] + pair[c, k]
            copy = remote(
                partial.at[c, k - 1], across.at[c, k - 1],
                across_send.at[c, k - 1], across_recv.at[c, k - 1],
                {"yr": chip_at[k] * 2 + core},
            )
            copy.start()
            crossing.append(copy)

    def col(c, i):
        block = got.at[c, sta]
        return remote(
            block, block, col_send.at[c, i], col_recv.at[c, row],
            {"sta": rows_by[i] * minor + place},
        )

    def relay(c):
        block = got.at[c, rows_by[-1] * minor + place]
        return remote(
            block, block, col_send.at[c, major - 1], col_recv.at[c, rows_by[-1]],
            {"sta": rows_by[0] * minor + place},
        )

    def turn(c, j):
        block = got.at[c, row * minor + lax.rem(place + minor - j, minor)]
        return remote(
            block, block, row_send.at[c, rows_by[0], j - 1], row_recv.at[c, row, j - 1],
            {"sta": rows_by[0] * minor + place},
        )

    def col_in(c, i):
        block = got.at[c, rows_by[i] * minor + place]
        return remote(
            block, block, col_send.at[c, i], col_recv.at[c, rows_by[i]],
            {"sta": rows_by[i] * minor + place},
        )

    def across_row(c, from_row, j):
        block = got.at[c, from_row * minor + place]
        return remote(
            block, block, row_send.at[c, from_row, j - 1], row_recv.at[c, from_row, j - 1],
            {"sta": row * minor + lax.rem(place + j, minor)},
        )

    def row_in(c, from_row, j):
        block = got.at[c, from_row * minor + lax.rem(place + minor - j, minor)]
        return remote(
            block, block, row_send.at[c, from_row, j - 1], row_recv.at[c, from_row, j - 1],
            {"sta": row * minor + lax.rem(place + minor - j, minor)},
        )

    def own(c):
        pairs[c * chips + chips - 1].wait_recv()
        total = sums_ref[yr, c] + pair[c, 0]
        for k in range(chips - 1):
            crossing[c * (chips - 1) + k].wait_recv()
            total = total + across[c, k]
        got[c, sta] = total
        for i in range(major - 1):
            if relayed and i == major - 2:
                pl.when(inner)(col(c, i).start)
            else:
                col(c, i).start()
        for j in range(1, minor):
            across_row(c, row, j).start()

    def forward(c, then=lambda i: None):
        for i in range(major - 1):
            then(i)
            col_in(c, i).wait_recv()
            if relayed and i == major - 2:
                pl.when(inner)(relay(c).start)
            for j in range(1, minor):
                if turned[c] and i == 0:
                    row_in(c, row, j).wait_recv()
                    turn(c, j).start()
                else:
                    across_row(c, rows_by[i], j).start()
        then(major - 1)

    first = sta * cell_dev
    own_ids = [cells_ref[h : h + 1] for h in range(halves)]

    def targets():
        if not cap:
            lane = iota((1, slots), 1)
            return jnp.concatenate([jnp.where(lane < cell_dev, lane + first, -1)] + own_ids, axis=1)
        local = jnp.concatenate([ids[s, :halves] for s in range(owners)], axis=0) - first
        owned = (local >= 0) & (local < cell_dev)
        flags = one_where(owned)
        tile = (LANES, LANES)
        rank = dot(flags, one_where(iota(tile, 0) < iota(tile, 1)))
        held = dot(flags, jnp.ones(tile, BF16))
        ranks = []
        for s in range(owners):
            for h in range(halves):
                at = s * halves + h
                ranks.append(sum([held[s * halves + g : s * halves + g + 1] for g in range(h)],
                                 rank[at : at + 1]))
        ranks = jnp.where(owned, jnp.concatenate(ranks, axis=0), -1.0).T
        high, low = (local >> 8).astype(F32), (local & 255).astype(F32)
        lane = iota((LANES, cap), 1).astype(F32)
        found = []
        for s in range(owners):
            at = s * halves
            place = jnp.concatenate(
                [one_where(ranks[:, at + h : at + h + 1] == lane) for h in range(halves)], axis=0
            )
            line = [
                jnp.concatenate([part[at + h : at + h + 1] for h in range(halves)], axis=1)
                for part in (high, low)
            ]
            line.append(jnp.ones_like(line[0]))
            line.append(jnp.zeros((TILE - 3, stations), F32))
            got_line = dot(jnp.concatenate(line, axis=0).astype(BF16), place)
            number = 256.0 * got_line[0:1] + got_line[1:2]
            found.append(jnp.where(got_line[2:3] > 0.5, number, -1.0))
        column = jnp.concatenate(found, axis=0).T
        lane = iota((1, cell_pad), 1).astype(F32)
        for s in range(owners):
            unpack[s * cap : (s + 1) * cap] = one_where(column[:, s : s + 1] == lane)
        known = jnp.concatenate(found, axis=1).astype(I32)
        known = jnp.where(known >= 0, known + first, -1)
        return jnp.concatenate([known] + own_ids, axis=1)

    def build(target, low, high):
        for s in range(low, high):
            column = ids[s].T
            for h in range(halves):
                at = s * stations + h * LANES
                hot[at : at + LANES] = one_where(column[:, h : h + 1] == target)

    def cells(c):
        for j in range(1, minor):
            if not turned[c]:
                row_in(c, row, j).wait_recv()
            for i in range(major - 1):
                row_in(c, rows_by[i], j).wait_recv()
        for s in range(owners):
            sums = [got[c, s, k] for k in range(3)]
            high = [v.astype(BF16).astype(F32) for v in sums]
            low = [v - h for v, h in zip(sums, high)]
            tallies = [None] * 3
            for w, held in enumerate(words):
                word = got[c, s, 3 + w].astype(I32)
                for p, k in enumerate(held):
                    tallies[k] = ((word // base**p) & (base - 1)).astype(F32)
            parts = high + low + tallies
            if base > 256:
                rounded = [t.astype(BF16).astype(F32) for t in tallies]
                parts = high + low + rounded + [t - r for t, r in zip(tallies, rounded)]
            if len(parts) % 2:
                parts.append(jnp.zeros_like(parts[0]))
            lhs[:, s * stations : (s + 1) * stations] = jnp.concatenate(parts, axis=0).astype(BF16)
        total = dot(lhs[...], hot[...])
        step = 3 * TILE
        tally = total[2 * step : 3 * step]
        if base > 256:
            tally = tally + total[3 * step : 4 * step]
        clim = (total[:step] + total[step : 2 * step]) / jnp.maximum(tally, 1.0)
        clim_ref[yr, c] = clim.reshape(3, TILE, width)
        for k in range(1, chips):
            far(c, k).start()
        near(c, 0).start()

    def far(c, k):
        block = clim_ref.at[yr, c]
        return remote(
            block, block, far_send.at[c, k - 1], far_recv.at[c, k - 1],
            {"yr": chip_at[k] * 2 + core},
        )

    def near(c, k):
        block = clim_ref.at[chip_from[k] * 2 + core, c]
        return remote(block, block, near_send.at[c, k], near_recv.at[c, k], partner)

    def hand_on(c):
        for k in range(1, chips):
            far(c, k).wait_recv()
            near(c, k).start()

    def expand(c):
        for k in range(chips):
            near(c, k).wait_recv()
        both = clim_ref[:, c]
        out_ref[:, c, :, :, cell_pad:] = both[..., slots:]
        flat = both[..., :slots].reshape(ranges * 3 * TILE, slots)
        if not cap:
            out_ref[:, c, :, :, :cell_pad] = both[..., :slots]
            return
        rows = flat.shape[0]
        ones = jnp.ones((2 * TILE, slots), BF16)
        wide = dot(jnp.concatenate([*split_two(flat), ones], axis=0), unpack[...])
        times = jnp.maximum(wide[2 * rows : 2 * rows + 1], 1.0)
        cells_at = (wide[:rows] + wide[rows : 2 * rows]) / times
        out_ref[:, c, :, :, :cell_pad] = cells_at.reshape(ranges, 3, TILE, cell_pad)

    own(0)
    for copy in id_copies:
        copy.wait_recv()
    target = targets()
    for c in range(1, chunks):
        own(c)
    share = -(-owners // major)
    forward(0, lambda i: build(target, i * share, min((i + 1) * share, owners)))
    for c in range(chunks):
        if c + 1 < chunks:
            forward(c + 1)
        cells(c)
        if c >= 2:
            hand_on(c - 2)
        if c >= 3:
            expand(c - 3)
    for c in range(max(chunks - 2, 0), chunks):
        hand_on(c)
    for c in range(max(chunks - 3, 0), chunks):
        expand(c)
    for c in range(chunks):
        for k in range(chips):
            near(c, k).wait_send()
        for k in range(1, chips):
            far(c, k).wait_send()
        for i in range(major - 1):
            if relayed and i == major - 2:
                pl.when(inner)(col(c, i).wait_send)
                pl.when(inner)(relay(c).wait_send)
            else:
                col(c, i).wait_send()
        for j in range(1, minor):
            across_row(c, row, j).wait_send()
            for i in range(major - 1):
                across_row(c, rows_by[i], j).wait_send()
    for copy in id_copies + pairs + crossing:
        copy.wait_send()


def anomaly_kernel(
    ranges, cell_dev, cell_pad, rows, masked_ref, code_ref, clim_ref,
    out_hbm, climatology_hbm, table, clim_buf, out_buf, clim_sem, out_sem,
):
    block_total, days = masked_ref.shape
    stations = clim_ref.shape[-1] - cell_pad
    steps = block_total // rows
    low, high = [], []
    for i in range(steps):
        ends = [code_ref[at : at + TILE] for at in (i * rows, (i + 1) * rows - TILE)]
        low.append((jnp.min(ends[0]) >> 1) // (3 * GROUP))
        high.append((jnp.max(ends[1]) >> 1) // (3 * GROUP))
    close = functools.reduce(jnp.logical_and, [h - l < WINDOW // (3 * GROUP) for l, h in zip(low, high)])
    for k in range(3):
        part = clim_ref[:, :, k, :, cell_pad:].reshape(days, stations).T
        both = jnp.concatenate(split_two(part), axis=1)
        for g in range(stations // GROUP):
            at = (3 * g + k) * GROUP
            table[at : at + GROUP] = both[g * GROUP : (g + 1) * GROUP]
    table[3 * stations :] = jnp.zeros((table.shape[0] - 3 * stations, 2 * days), BF16)
    clim_copy = pltpu.make_async_copy(clim_buf, climatology_hbm, clim_sem.at[0])
    copies = [
        pltpu.make_async_copy(
            out_buf.at[i * rows : (i + 1) * rows], out_hbm.at[i * rows : (i + 1) * rows], out_sem.at[i]
        )
        for i in range(steps)
    ]
    for j in range(cell_pad // LANES):
        for k in range(3):
            part = clim_ref[:, :, k, :, j * LANES : (j + 1) * LANES].reshape(days, LANES)
            last = min((j + 1) * LANES, cell_dev)
            clim_buf[j * LANES : last, k * days : (k + 1) * days] = part.T[: last - j * LANES]
    clim_copy.start()

    def subtract(windows_of):
        lane = iota((rows, LANES), 1)
        for i in range(steps):
            here = slice(i * rows, (i + 1) * rows)
            code = code_ref[here]
            segment = code >> 1
            found = None
            for start in windows_of(i):
                place = segment - start
                hot = jnp.concatenate(
                    [one_where(place == lane + j) for j in range(0, WINDOW, LANES)], axis=1
                )
                part = dot(hot, table[pl.ds(start, WINDOW)])
                found = part if found is None else found + part
            clim = found[:, :days] + found[:, days:]
            out_buf[here] = masked_ref[here] - (code & 1).astype(F32) * clim
            copies[i].start()

    @pl.when(close)
    def _():
        subtract(lambda i: [pl.multiple_of(low[i] * (3 * GROUP), GROUP)])

    @pl.when(jnp.logical_not(close))
    def _():
        subtract(lambda i: range(0, 3 * stations, WINDOW))

    for copy in [clim_copy] + copies:
        copy.wait()


def per_device(temps, day_bits, block_offset, block_counts, station_cell):
    owners, ranges = lax.axis_size("sta"), lax.axis_size("yr")
    stations = station_cell.shape[0]
    block_total, days = temps.shape
    cell_dev = CELLS // owners
    cell_pad = round_up(cell_dev, LANES)
    width = cell_pad + stations
    words, base = tally_words(ranges)
    groups = 3 + len(words)
    chunks = days // ranges // TILE
    rows = 1024 if block_total % 1024 == 0 else block_total
    cap = 4 * stations // owners
    if cap % LANES or owners * cap >= cell_pad:
        cap = 0
    slots = owners * cap if cap else cell_pad
    major = 4 if owners % 4 == 0 else owners
    minor, chips = owners // major, ranges // 2
    dma = pltpu.SemaphoreType.DMA
    whole = pl.BlockSpec(memory_space=VMEM)
    hbm = pl.BlockSpec(memory_space=pltpu.HBM)

    inputs = [
        pltpu.with_memory_space_constraint(array, pltpu.HBM)
        for array in (
            temps, day_bits, block_offset.reshape(block_total // LANES, LANES), block_counts,
            station_cell.reshape(stations // LANES, LANES),
        )
    ]
    sums, masked, code, cells = pl.pallas_call(
        functools.partial(sums_kernel, ranges, rows),
        in_specs=[hbm] * 5,
        out_specs=[whole] * 4,
        out_shape=[
            jax.ShapeDtypeStruct((ranges, chunks, groups, TILE, stations), F32),
            jax.ShapeDtypeStruct((block_total, days), F32),
            jax.ShapeDtypeStruct((block_total, days), I32),
            jax.ShapeDtypeStruct((TILE, LANES), I32),
        ],
        scratch_shapes=[
            VMEM((day_bits.shape[0], block_total), I32),
            VMEM((block_total // LANES, LANES), I32),
            VMEM((1, stations), I32),
            VMEM((round_up(3 * stations, WINDOW) + WINDOW, 2 * days), F32),
            VMEM((len(words), stations + 2 * NEARBY, days), F32),
            dma((4,)), dma((block_total // rows,)),
        ],
        compiler_params=pltpu.CompilerParams(vmem_limit_bytes=40 * 1024 * 1024),
    )(*inputs)

    block = (groups, TILE, stations)
    parts = 3 * 3 if base <= 256 else 3 * 4
    crossings, sides = max(chips - 1, 1), max(minor - 1, 1)
    clim = pl.pallas_call(
        functools.partial(exchange_kernel, ranges, owners, major, cap, cell_dev, cell_pad),
        in_specs=[whole] * 2,
        out_specs=whole,
        out_shape=jax.ShapeDtypeStruct((ranges, chunks, 3, TILE, width), F32),
        scratch_shapes=[
            VMEM((owners, TILE, LANES), I32),
            VMEM((chunks, chips) + block, F32),
            VMEM((chunks, crossings) + block, F32),
            VMEM((chunks, crossings) + block, F32),
            VMEM((chunks, owners) + block, F32),
            VMEM((round_up(parts * TILE, 16), owners * stations), BF16),
            VMEM((owners * stations, slots + stations), BF16),
            VMEM((ranges, chunks, 3, TILE, slots + stations), F32),
            VMEM((slots, cell_pad) if cap else (2 * TILE, LANES), BF16),
            dma((owners - 1,)), dma((owners - 1,)),
            dma((chunks, chips)), dma((chunks, chips)),
            dma((chunks, crossings)), dma((chunks, crossings)),
            dma((chunks, major)), dma((chunks, major)),
            dma((chunks, major, sides)), dma((chunks, major, sides)),
            dma((chunks, crossings)), dma((chunks, crossings)),
            dma((chunks, chips)), dma((chunks, chips)),
        ],
        compiler_params=pltpu.CompilerParams(
            collective_id=0, has_side_effects=True, vmem_limit_bytes=40 * 1024 * 1024
        ),
    )(sums, cells)

    rows = 512 if block_total % 512 == 0 else block_total
    return pl.pallas_call(
        functools.partial(anomaly_kernel, ranges, cell_dev, cell_pad, rows),
        in_specs=[whole] * 3,
        out_specs=[hbm] * 2,
        out_shape=[
            jax.ShapeDtypeStruct((block_total, days), F32),
            jax.ShapeDtypeStruct((cell_dev, 3 * days), F32),
        ],
        scratch_shapes=[
            VMEM((round_up(3 * stations, WINDOW) + WINDOW, 2 * days), BF16),
            VMEM((cell_dev, 3 * days), F32),
            VMEM((block_total, days), F32),
            dma((1,)), dma((block_total // rows,)),
        ],
        compiler_params=pltpu.CompilerParams(vmem_limit_bytes=40 * 1024 * 1024),
    )(masked, code, clim)


def solution(mesh):
    in_specs = (
        P(("sta", "yr"), None),
        P(None, ("sta", "yr")),
        P(("sta", "yr")),
        P("yr", "sta"),
        P("sta"),
    )
    out_specs = (P(("sta", "yr"), None), P("sta", None))

    def run(*args):
        return tuple(per_device(*args))

    return jax.shard_map(
        run, mesh=mesh, in_specs=in_specs, out_specs=out_specs, check_vma=False
    )
```

```python
import functools

import jax
import jax.numpy as jnp
from jax import lax
from jax.experimental import pallas as pl
from jax.experimental.pallas import tpu as pltpu
from jax.sharding import PartitionSpec as P

CELLS = 10368
CALENDAR = 365
MOST_BLOCKS = 48
LANES = 128
TILE = 8
GROUP = 16
WINDOW = 256
NEARBY = 96
F32 = jnp.float32
BF16 = jnp.bfloat16
I32 = jnp.int32
VMEM = pltpu.VMEM


def round_up(value, step):
    return (value + step - 1) // step * step


def tally_words(ranges):
    if ranges * MOST_BLOCKS < 256:
        return [(0, 1, 2)], 256
    return [(0, 1), (2,)], 4096


def iota(shape, dim):
    return lax.broadcasted_iota(I32, shape, dim)


def one_where(mask):
    return jnp.where(mask, 1.0, 0.0).astype(BF16)


def dot(a, b, dims=((1,), (0,))):
    return lax.dot_general(a, b, (dims, ((), ())), preferred_element_type=F32)


def split_two(value):
    high = value.astype(BF16)
    return high, (value - high.astype(F32)).astype(BF16)


def row_stations(counts, blocks):
    stations = counts.shape[1]
    spread = jnp.broadcast_to(counts.astype(F32), (LANES, stations)).astype(BF16)
    square = (stations, stations)
    ends = dot(one_where(iota(square, 1) <= iota(square, 0)), spread, ((1,), (1,))).astype(I32)
    lane = iota((stations, LANES), 1)
    ending = dot(one_where((ends >> 7) == lane), one_where((ends & 127) == lane), ((0,), (0,)))
    ending = ending.astype(BF16)
    tile = (LANES, LANES)
    within = dot(ending, one_where(iota(tile, 0) <= iota(tile, 1)))
    totals = dot(ending, jnp.ones(tile, BF16)).astype(BF16)
    before = dot(one_where(iota(tile, 1) < iota(tile, 0)), totals)
    return (within + before)[:blocks]


def sums_kernel(
    ranges, rows, temps_hbm, bits_hbm, offs_hbm, counts_hbm, cell_hbm,
    sums_ref, masked_ref, code_ref, cells_ref, bits, offs, counts, acc, tally, small, large,
):
    block_total = masked_ref.shape[0]
    blocks, stations = offs.shape[0], counts.shape[1]
    words, base = tally_words(ranges)
    chunk_count = sums_ref.shape[1]
    firsts = [
        pltpu.make_async_copy(counts_hbm, counts, small.at[0]),
        pltpu.make_async_copy(offs_hbm, offs, small.at[1]),
        pltpu.make_async_copy(bits_hbm, bits, small.at[2]),
        pltpu.make_async_copy(cell_hbm, cells_ref.at[0 : cell_hbm.shape[0]], small.at[3]),
    ]
    steps = block_total // rows
    loads = [
        pltpu.make_async_copy(
            temps_hbm.at[i * rows : (i + 1) * rows], masked_ref.at[i * rows : (i + 1) * rows],
            large.at[i],
        )
        for i in range(steps)
    ]
    for copy in firsts + loads:
        copy.start()
    firsts[0].wait()
    station = row_stations(counts[...], blocks)
    firsts[1].wait()
    offsets = offs[...]
    third = offsets - 3 * ((offsets * 21846) >> 16)
    station = station.astype(I32)
    segment = (station // GROUP) * (3 * GROUP) + third * GROUP + station % GROUP
    double_segment = 2 * segment
    limit = CALENDAR - LANES * third
    weight_of = []
    for held in words:
        weight = jnp.zeros(third.shape, F32)
        for place, k in enumerate(held):
            weight = jnp.where(third == k, float(base**place), weight)
        weight_of.append(weight.astype(BF16))
    group = station // GROUP
    per_step = rows // LANES
    low = [jnp.min(group[i * per_step : (i + 1) * per_step]) for i in range(steps)]
    high = [jnp.max(group[i * per_step : (i + 1) * per_step]) for i in range(steps)]
    close = functools.reduce(jnp.logical_and, [h - l < WINDOW // (3 * GROUP) for l, h in zip(low, high)])
    at = iota((WINDOW, LANES), 0).astype(F32).astype(BF16)
    day = iota((LANES, LANES), 0)
    shift = day & 31
    one, zero = jnp.ones((), BF16), jnp.zeros((), BF16)
    acc[...] = jnp.zeros_like(acc)
    tally[...] = jnp.zeros_like(tally)
    firsts[2].wait()
    for q in range(blocks):
        here = slice(q * LANES, (q + 1) * LANES)
        packed = jnp.concatenate(
            [jnp.broadcast_to(bits[w : w + 1, here], (32, LANES)) for w in range(bits.shape[0])],
            axis=0,
        )
        bit = (packed >> shift) & 1
        code = jnp.where(day < limit[q : q + 1], bit, 0) + double_segment[q : q + 1]
        code_ref[here] = code.T
    for copy in loads:
        copy.wait()

    def against(number, start, size):
        return jnp.clip(number - start, -1, size).astype(F32).astype(BF16)

    def spread(lines, q, size):
        return jnp.broadcast_to(lines[q : q + 1], (size, LANES))

    def add_up(windows_of, nearby_of):
        for i in range(steps):
            values, observed_all = [], []
            blocks_here = range(i * per_step, (i + 1) * per_step)
            for q in blocks_here:
                here = slice(q * LANES, (q + 1) * LANES)
                observed = (code_ref[here] & 1).astype(F32)
                value = masked_ref[here] * observed
                masked_ref[here] = value
                values.append(jnp.concatenate(split_two(value), axis=1))
                observed_all.append(observed.astype(BF16))
            values = jnp.concatenate(values, axis=0)
            observed_all = jnp.concatenate(observed_all, axis=0)
            for start in windows_of(i):
                place = against(segment, start, WINDOW)
                hot = jnp.concatenate(
                    [jnp.where(at == spread(place, q, WINDOW), one, zero) for q in blocks_here], axis=1
                )
                acc[pl.ds(start, WINDOW)] += dot(hot, values)
            for start in nearby_of(i):
                place = against(station, start, NEARBY)
                for w, weight in enumerate(weight_of):
                    hot = jnp.concatenate(
                        [
                            jnp.where(
                                at[:NEARBY] == spread(place, q, NEARBY), spread(weight, q, NEARBY), zero
                            )
                            for q in blocks_here
                        ],
                        axis=1,
                    )
                    tally[w, pl.ds(start, NEARBY)] += dot(hot, observed_all)

    @pl.when(close)
    def _():
        add_up(
            lambda i: [pl.multiple_of(low[i] * (3 * GROUP), GROUP)],
            lambda i: [pl.multiple_of(low[i] * GROUP, GROUP)],
        )

    @pl.when(jnp.logical_not(close))
    def _():
        add_up(
            lambda i: range(0, 3 * stations, WINDOW), lambda i: range(0, stations, NEARBY)
        )

    split = (ranges, chunk_count, TILE, stations)
    for k in range(3):
        part = jnp.concatenate(
            [
                acc[(3 * g + k) * GROUP : (3 * g + k + 1) * GROUP]
                for g in range(stations // GROUP)
            ],
            axis=0,
        )
        sums_ref[:, :, k] = (part[:, :LANES] + part[:, LANES:]).T.reshape(split)
    for w in range(len(words)):
        sums_ref[:, :, 3 + w] = tally[w, :stations].T.reshape(split)
    firsts[3].wait()


def remote(src, dst, send, recv, where):
    return pltpu.make_async_remote_copy(
        src_ref=src, dst_ref=dst, send_sem=send, recv_sem=recv,
        device_id=where, device_id_type=pl.DeviceIdType.MESH,
    )


def signal(semaphore, where):
    pl.semaphore_signal(semaphore, inc=1, device_id=where, device_id_type=pl.DeviceIdType.MESH)


def pick(index, table):
    value = jnp.int32(table[0])
    for i in range(1, len(table)):
        value = jnp.where(index == i, jnp.int32(table[i]), value)
    return value


def exchange_kernel(
    ranges, owners, major, cell_dev, cell_pad, sums_ref, cells_ref, clim_ref,
    ids, pair, partial, across, got, lhs, started, hot,
    ready, further, pair_send, pair_recv, across_send, across_recv,
    col_send, col_recv, row_send, row_recv, far_send, far_recv, near_send, near_recv,
):
    _, chunks, groups, _, stations = sums_ref.shape
    halves = stations // LANES
    words, base = tally_words(ranges)
    base_bits = base.bit_length() - 1
    width = clim_ref.shape[-1]
    slots = width - stations
    chips, minor = ranges // 2, owners // major
    sta, yr = lax.axis_index("sta"), lax.axis_index("yr")
    chip, core = yr // 2, lax.rem(yr, 2)
    row, place = sta // minor, lax.rem(sta, minor)
    partner = {"yr": chip * 2 + 1 - core}
    chip_at = [lax.rem(chip + k, chips) for k in range(chips)]
    chip_from = [lax.rem(chip + chips - k, chips) for k in range(chips)]
    near_first = [
        sorted(
            (r for r in range(major) if r != mine),
            key=lambda r: (abs(r - mine), r if 2 * mine < major else -r),
        )
        for mine in range(major)
    ]
    relayed = major == 4
    inner = (row == 1) | (row == 2)
    relays = [relayed and 0 < c < chunks for c in range(chunks + 1)]
    turned = [relayed and c % 2 == 1 for c in range(chunks)] + [False]
    rows_by = [pick(row, [near_first[m][i] for m in range(major)]) for i in range(major - 1)]

    barrier = pltpu.get_barrier_semaphore()
    beside = [{"sta": row * minor + lax.rem(place + j, minor)} for j in range(1, minor)]
    near_peers = [partner] + [{"yr": c * 2 + core} for c in chip_at[1:]] + beside
    steps_by = [(row > 0, row - 1), (row < major - 1, row + 1)] if relayed else []
    if not relayed:
        near_peers += [{"sta": r * minor + place} for r in rows_by]
    for where in near_peers:
        signal(barrier, where)
    neighbours = pick(row, [1] + [2] * (major - 2) + [1]) if relayed else 0
    for able, to_row in steps_by:
        pl.when(able)(functools.partial(signal, barrier, {"sta": to_row * minor + place}))
    pl.semaphore_wait(barrier, len(near_peers) + neighbours)
    for able, to_row in steps_by:
        pl.when(able)(functools.partial(signal, ready, {"sta": to_row * minor + place}))
    def view(c, owner):
        return got.at[c, owner] if c < chunks else ids.at[owner]

    def send_own(c, which):
        for i in which:
            if relays[c] and i == major - 2:
                pl.when(inner)(col(c, i).start)
            else:
                col(c, i).start()

    def col(c, i):
        block = view(c, sta)
        return remote(
            block, block, col_send.at[c, i], col_recv.at[c, row],
            {"sta": rows_by[i] * minor + place},
        )

    def relay(c):
        block = view(c, rows_by[-1] * minor + place)
        return remote(
            block, block, col_send.at[c, major - 1], col_recv.at[c, rows_by[-1]],
            {"sta": rows_by[0] * minor + place},
        )

    def turn(c, j):
        block = view(c, row * minor + lax.rem(place + minor - j, minor))
        return remote(
            block, block, row_send.at[c, rows_by[0], j - 1], row_recv.at[c, row, j - 1],
            {"sta": rows_by[0] * minor + place},
        )

    def col_in(c, i):
        block = view(c, rows_by[i] * minor + place)
        return remote(
            block, block, col_send.at[c, i], col_recv.at[c, rows_by[i]],
            {"sta": rows_by[i] * minor + place},
        )

    def across_row(c, from_row, j):
        block = view(c, from_row * minor + place)
        return remote(
            block, block, row_send.at[c, from_row, j - 1], row_recv.at[c, from_row, j - 1],
            {"sta": row * minor + lax.rem(place + j, minor)},
        )

    def row_in(c, from_row, j):
        block = view(c, from_row * minor + lax.rem(place + minor - j, minor))
        return remote(
            block, block, row_send.at[c, from_row, j - 1], row_recv.at[c, from_row, j - 1],
            {"sta": row * minor + lax.rem(place + minor - j, minor)},
        )

    pairs = []
    for c in range(chunks):
        for k in [*range(1, chips), 0]:
            copy = remote(
                sums_ref.at[chip_at[k] * 2 + 1 - core, c], pair.at[c, k],
                pair_send.at[c, k], pair_recv.at[c, k], partner,
            )
            copy.start()
            pairs.append(copy)
    ids[sta] = cells_ref[...]
    send_own(chunks, [0])
    for j in range(1, minor):
        across_row(chunks, row, j).start()
    crossing = []
    for c in range(chunks):
        for k in range(1, chips):
            pairs[c * chips + k - 1].wait_recv()
            partial[c, k - 1] = sums_ref[chip_at[k] * 2 + core, c] + pair[c, k]
            copy = remote(
                partial.at[c, k - 1], across.at[c, k - 1],
                across_send.at[c, k - 1], across_recv.at[c, k - 1],
                {"yr": chip_at[k] * 2 + core},
            )
            copy.start()
            crossing.append(copy)

    def own(c):
        pairs[c * chips + chips - 1].wait_recv()
        total = sums_ref[yr, c] + pair[c, 0]
        for k in range(chips - 1):
            crossing[c * (chips - 1) + k].wait_recv()
            total = total + across[c, k]
        got[c, sta] = total
        send_own(c, range(major - 1))
        for j in range(1, minor):
            across_row(c, row, j).start()

    def pass_on(c, i):
        col_in(c, i).wait_recv()
        if relays[c] and i == major - 2:
            pl.when(inner)(relay(c).start)
        for j in range(1, minor):
            if turned[c] and i == 0:
                row_in(c, row, j).wait_recv()
                turn(c, j).start()
            else:
                across_row(c, rows_by[i], j).start()

    def forward(c):
        for i in range(major - 1):
            pass_on(c, i)

    def side_in(c):
        for j in range(1, minor):
            if not turned[c]:
                row_in(c, row, j).wait_recv()
            for i in range(major - 1):
                row_in(c, rows_by[i], j).wait_recv()

    owner_at = [
        r * minor + lax.rem(place + j, minor) for j in range(minor) for r in [row] + rows_by
    ]

    first = sta * cell_dev
    own_ids = [cells_ref[h : h + 1] for h in range(halves)]

    lane = iota((1, slots), 1)
    target = jnp.concatenate([jnp.where(lane < cell_dev, lane + first, -1)] + own_ids, axis=1)

    def build(low, high):
        for s in range(low, high):
            column = ids[owner_at[s]].T
            for h in range(halves):
                at = s * stations + h * LANES
                hot[at : at + LANES] = one_where(column[:, h : h + 1] == target)

    def add_shards(c, low, high):
        for s in range(low, high):
            owner = owner_at[s]
            sums = [got[c, owner, k] for k in range(3)]
            high_part = [v.astype(BF16).astype(F32) for v in sums]
            low_part = [v - h for v, h in zip(sums, high_part)]
            tallies = [None] * 3
            for w, held in enumerate(words):
                word = got[c, owner, 3 + w].astype(I32)
                for p, k in enumerate(held):
                    tallies[k] = ((word >> (p * base_bits)) & (base - 1)).astype(F32)
            parts = high_part + low_part + tallies
            if base > 256:
                rounded = [t.astype(BF16).astype(F32) for t in tallies]
                parts = high_part + low_part + rounded + [t - r for t, r in zip(tallies, rounded)]
            if len(parts) % 2:
                parts.append(jnp.zeros_like(parts[0]))
            lhs[:, s * stations : (s + 1) * stations] = jnp.concatenate(parts, axis=0).astype(BF16)
        here = slice(low * stations, high * stations)
        return dot(lhs[:, here], hot[here])

    def cells_start(c):
        started[...] = add_shards(c, 0, major)

    def cells(c):
        side_in(c)
        total = started[...] + add_shards(c, major, owners) if minor > 1 else started[...]
        step = 3 * TILE
        tally = total[2 * step : 3 * step]
        if base > 256:
            tally = tally + total[3 * step : 4 * step]
        clim = (total[:step] + total[step : 2 * step]) / jnp.maximum(tally, 1.0)
        clim_ref[yr, c] = clim.reshape(3, TILE, width)
        for k in range(1, chips):
            far(c, k).start()
        near(c, 0).start()

    def far(c, k):
        block = clim_ref.at[yr, c]
        return remote(
            block, block, far_send.at[c, k - 1], far_recv.at[c, k - 1],
            {"yr": chip_at[k] * 2 + core},
        )

    def near(c, k):
        block = clim_ref.at[chip_from[k] * 2 + core, c]
        return remote(block, block, near_send.at[c, k], near_recv.at[c, k], partner)

    def hand_on(c):
        for k in range(1, chips):
            far(c, k).wait_recv()
            near(c, k).start()

    if relayed:
        pl.semaphore_wait(ready, neighbours)
        for able, to_row in steps_by:
            pl.when(able)(functools.partial(signal, further, {"sta": to_row * minor + place}))
        pl.semaphore_wait(further, neighbours)
    send_own(chunks, range(1, major - 1))
    last = major - 2
    for c in range(min(chunks, 2)):
        own(c)
        if c < last:
            pass_on(chunks, c)
    for i in range(min(chunks, 2, last), last + 1):
        pass_on(chunks, i)
    for i in range(last):
        pass_on(0, i)
    if chunks > 2:
        own(2)
    build(0, last + 1)
    pass_on(0, last)
    for c in range(3, chunks):
        own(c)
    build(last + 1, major)
    cells_start(0)
    if chunks > 1:
        for i in range(major - 2):
            pass_on(1, i)
    side_in(chunks)
    build(major, owners)
    if chunks > 1:
        pass_on(1, major - 2)
    for c in range(chunks):
        if c > 0 and c + 1 < chunks:
            forward(c + 1)
        cells(c)
        if c + 1 < chunks:
            cells_start(c + 1)
        if c >= 2:
            hand_on(c - 2)
    for c in range(max(chunks - 2, 0), chunks):
        hand_on(c)
    for c in range(chunks):
        for k in range(chips):
            near(c, k).wait()
        for k in range(1, chips):
            far(c, k).wait_send()
    for c in range(chunks + 1):
        for i in range(major - 1):
            if relays[c] and i == major - 2:
                pl.when(inner)(col(c, i).wait_send)
                pl.when(inner)(relay(c).wait_send)
            else:
                col(c, i).wait_send()
        for j in range(1, minor):
            across_row(c, row, j).wait_send()
            for i in range(major - 1):
                across_row(c, rows_by[i], j).wait_send()
    for copy in pairs + crossing:
        copy.wait_send()


def anomaly_kernel(
    ranges, cell_dev, cell_pad, rows, masked_ref, code_ref, clim_ref,
    out_hbm, climatology_hbm, table, clim_buf, out_buf, clim_sem, out_sem,
):
    block_total, days = masked_ref.shape
    stations = clim_ref.shape[-1] - cell_pad
    steps = block_total // rows
    low, high = [], []
    for i in range(steps):
        ends = [code_ref[at : at + TILE] for at in (i * rows, (i + 1) * rows - TILE)]
        low.append((jnp.min(ends[0]) >> 1) // (3 * GROUP))
        high.append((jnp.max(ends[1]) >> 1) // (3 * GROUP))
    close = functools.reduce(jnp.logical_and, [h - l < WINDOW // (3 * GROUP) for l, h in zip(low, high)])
    for k in range(3):
        part = clim_ref[:, :, k, :, cell_pad:].reshape(days, stations).T
        both = jnp.concatenate(split_two(part), axis=1)
        for g in range(stations // GROUP):
            at = (3 * g + k) * GROUP
            table[at : at + GROUP] = both[g * GROUP : (g + 1) * GROUP]
    table[3 * stations :] = jnp.zeros((table.shape[0] - 3 * stations, 2 * days), BF16)
    clim_copy = pltpu.make_async_copy(clim_buf, climatology_hbm, clim_sem.at[0])
    copies = [
        pltpu.make_async_copy(
            out_buf.at[i * rows : (i + 1) * rows], out_hbm.at[i * rows : (i + 1) * rows], out_sem.at[i]
        )
        for i in range(steps)
    ]
    for j in range(cell_pad // LANES):
        for k in range(3):
            part = clim_ref[:, :, k, :, j * LANES : (j + 1) * LANES].reshape(days, LANES)
            last = min((j + 1) * LANES, cell_dev)
            clim_buf[j * LANES : last, k * days : (k + 1) * days] = part.T[: last - j * LANES]
    clim_copy.start()

    def subtract(windows_of):
        lane = iota((rows, LANES), 1)
        for i in range(steps):
            here = slice(i * rows, (i + 1) * rows)
            code = code_ref[here]
            segment = code >> 1
            found = None
            for start in windows_of(i):
                place = segment - start
                hot = jnp.concatenate(
                    [one_where(place == lane + j) for j in range(0, WINDOW, LANES)], axis=1
                )
                part = dot(hot, table[pl.ds(start, WINDOW)])
                found = part if found is None else found + part
            clim = found[:, :days] + found[:, days:]
            out_buf[here] = masked_ref[here] - (code & 1).astype(F32) * clim
            copies[i].start()

    @pl.when(close)
    def _():
        subtract(lambda i: [pl.multiple_of(low[i] * (3 * GROUP), GROUP)])

    @pl.when(jnp.logical_not(close))
    def _():
        subtract(lambda i: range(0, 3 * stations, WINDOW))

    for copy in [clim_copy] + copies:
        copy.wait()


def per_device(temps, day_bits, block_offset, block_counts, station_cell):
    owners, ranges = lax.axis_size("sta"), lax.axis_size("yr")
    stations = station_cell.shape[0]
    block_total, days = temps.shape
    cell_dev = CELLS // owners
    cell_pad = round_up(cell_dev, LANES)
    width = cell_pad + stations
    words, base = tally_words(ranges)
    groups = 3 + len(words)
    chunks = days // ranges // TILE
    rows = 1024 if block_total % 1024 == 0 else block_total
    major = 4 if owners % 4 == 0 else owners
    minor, chips = owners // major, ranges // 2
    dma = pltpu.SemaphoreType.DMA
    whole = pl.BlockSpec(memory_space=VMEM)
    hbm = pl.BlockSpec(memory_space=pltpu.HBM)

    inputs = [
        pltpu.with_memory_space_constraint(array, pltpu.HBM)
        for array in (
            temps, day_bits, block_offset.reshape(block_total // LANES, LANES), block_counts,
            station_cell.reshape(stations // LANES, LANES),
        )
    ]
    sums, masked, code, cells = pl.pallas_call(
        functools.partial(sums_kernel, ranges, rows),
        in_specs=[hbm] * 5,
        out_specs=[whole] * 4,
        out_shape=[
            jax.ShapeDtypeStruct((ranges, chunks, groups, TILE, stations), F32),
            jax.ShapeDtypeStruct((block_total, days), F32),
            jax.ShapeDtypeStruct((block_total, days), I32),
            jax.ShapeDtypeStruct((TILE, LANES), I32),
        ],
        scratch_shapes=[
            VMEM((day_bits.shape[0], block_total), I32),
            VMEM((block_total // LANES, LANES), I32),
            VMEM((1, stations), I32),
            VMEM((round_up(3 * stations, WINDOW) + WINDOW, 2 * days), F32),
            VMEM((len(words), stations + 2 * NEARBY, days), F32),
            dma((4,)), dma((block_total // rows,)),
        ],
        compiler_params=pltpu.CompilerParams(vmem_limit_bytes=40 * 1024 * 1024),
    )(*inputs)

    block = (groups, TILE, stations)
    parts = 3 * 3 if base <= 256 else 3 * 4
    crossings, sides = max(chips - 1, 1), max(minor - 1, 1)
    clim = pl.pallas_call(
        functools.partial(exchange_kernel, ranges, owners, major, cell_dev, cell_pad),
        in_specs=[whole] * 2,
        out_specs=whole,
        out_shape=jax.ShapeDtypeStruct((ranges, chunks, 3, TILE, width), F32),
        scratch_shapes=[
            VMEM((owners, TILE, LANES), I32),
            VMEM((chunks, chips) + block, F32),
            VMEM((chunks, crossings) + block, F32),
            VMEM((chunks, crossings) + block, F32),
            VMEM((chunks, owners) + block, F32),
            VMEM((round_up(parts * TILE, 16), owners * stations), BF16),
            VMEM((round_up(parts * TILE, 16), width), F32),
            VMEM((owners * stations, width), BF16),
            pltpu.SemaphoreType.REGULAR, pltpu.SemaphoreType.REGULAR,
            dma((chunks, chips)), dma((chunks, chips)),
            dma((chunks, crossings)), dma((chunks, crossings)),
            dma((chunks + 1, major)), dma((chunks + 1, major)),
            dma((chunks + 1, major, sides)), dma((chunks + 1, major, sides)),
            dma((chunks, crossings)), dma((chunks, crossings)),
            dma((chunks, chips)), dma((chunks, chips)),
        ],
        compiler_params=pltpu.CompilerParams(
            collective_id=0, has_side_effects=True, vmem_limit_bytes=40 * 1024 * 1024
        ),
    )(sums, cells)

    rows = 512 if block_total % 512 == 0 else block_total
    return pl.pallas_call(
        functools.partial(anomaly_kernel, ranges, cell_dev, cell_pad, rows),
        in_specs=[whole] * 3,
        out_specs=[hbm] * 2,
        out_shape=[
            jax.ShapeDtypeStruct((block_total, days), F32),
            jax.ShapeDtypeStruct((cell_dev, 3 * days), F32),
        ],
        scratch_shapes=[
            VMEM((round_up(3 * stations, WINDOW) + WINDOW, 2 * days), BF16),
            VMEM((cell_dev, 3 * days), F32),
            VMEM((block_total, days), F32),
            dma((1,)), dma((block_total // rows,)),
        ],
        compiler_params=pltpu.CompilerParams(vmem_limit_bytes=40 * 1024 * 1024),
    )(masked, code, clim)


def solution(mesh):
    in_specs = (
        P(("sta", "yr"), None),
        P(None, ("sta", "yr")),
        P(("sta", "yr")),
        P("yr", "sta"),
        P("sta"),
    )
    out_specs = (P(("sta", "yr"), None), P("sta", None))

    def run(*args):
        return tuple(per_device(*args))

    return jax.shard_map(
        run, mesh=mesh, in_specs=in_specs, out_specs=out_specs, check_vma=False
    )
```

```python
import functools

import jax
import jax.numpy as jnp
from jax import lax
from jax.experimental import pallas as pl
from jax.experimental.pallas import tpu as pltpu
from jax.sharding import PartitionSpec as P

CELLS = 10368
CALENDAR = 365
MOST_BLOCKS = 48
LANES = 128
TILE = 8
GROUP = 16
WINDOW = 256
NEARBY = 96
F32 = jnp.float32
BF16 = jnp.bfloat16
I32 = jnp.int32
VMEM = pltpu.VMEM


def round_up(value, step):
    return (value + step - 1) // step * step


def tally_words(ranges):
    if ranges * MOST_BLOCKS < 256:
        return [(0, 1, 2)], 256
    return [(0, 1), (2,)], 4096


def iota(shape, dim):
    return lax.broadcasted_iota(I32, shape, dim)


def one_where(mask):
    return jnp.where(mask, 1.0, 0.0).astype(BF16)


def dot(a, b, dims=((1,), (0,))):
    return lax.dot_general(a, b, (dims, ((), ())), preferred_element_type=F32)


def split_two(value):
    high = value.astype(BF16)
    return high, (value - high.astype(F32)).astype(BF16)


def row_stations(counts, blocks):
    stations = counts.shape[1]
    spread = jnp.broadcast_to(counts.astype(F32), (LANES, stations)).astype(BF16)
    square = (stations, stations)
    ends = dot(one_where(iota(square, 1) <= iota(square, 0)), spread, ((1,), (1,))).astype(I32)
    lane = iota((stations, LANES), 1)
    ending = dot(one_where((ends >> 7) == lane), one_where((ends & 127) == lane), ((0,), (0,)))
    ending = ending.astype(BF16)
    tile = (LANES, LANES)
    within = dot(ending, one_where(iota(tile, 0) <= iota(tile, 1)))
    totals = dot(ending, jnp.ones(tile, BF16)).astype(BF16)
    before = dot(one_where(iota(tile, 1) < iota(tile, 0)), totals)
    return (within + before)[:blocks]


def sums_kernel(
    ranges, rows, temps_hbm, bits_hbm, offs_hbm, counts_hbm, cell_hbm,
    sums_ref, masked_ref, code_ref, cells_ref, bits, offs, counts, acc, tally, small, large,
):
    block_total = masked_ref.shape[0]
    blocks, stations = offs.shape[0], counts.shape[1]
    words, base = tally_words(ranges)
    chunk_count = sums_ref.shape[1]
    firsts = [
        pltpu.make_async_copy(counts_hbm, counts, small.at[0]),
        pltpu.make_async_copy(offs_hbm, offs, small.at[1]),
        pltpu.make_async_copy(bits_hbm, bits, small.at[2]),
        pltpu.make_async_copy(cell_hbm, cells_ref.at[0 : cell_hbm.shape[0]], small.at[3]),
    ]
    steps = block_total // rows
    loads = [
        pltpu.make_async_copy(
            temps_hbm.at[i * rows : (i + 1) * rows], masked_ref.at[i * rows : (i + 1) * rows],
            large.at[i],
        )
        for i in range(steps)
    ]
    for copy in firsts + loads:
        copy.start()
    firsts[0].wait()
    station = row_stations(counts[...], blocks)
    firsts[1].wait()
    offsets = offs[...]
    third = offsets - 3 * ((offsets * 21846) >> 16)
    station = station.astype(I32)
    segment = (station // GROUP) * (3 * GROUP) + third * GROUP + station % GROUP
    double_segment = 2 * segment
    limit = CALENDAR - LANES * third
    weight_of = []
    for held in words:
        weight = jnp.zeros(third.shape, F32)
        for place, k in enumerate(held):
            weight = jnp.where(third == k, float(base**place), weight)
        weight_of.append(weight.astype(BF16))
    group = station // GROUP
    per_step = rows // LANES
    low = [jnp.min(group[i * per_step : (i + 1) * per_step]) for i in range(steps)]
    high = [jnp.max(group[i * per_step : (i + 1) * per_step]) for i in range(steps)]
    close = functools.reduce(jnp.logical_and, [h - l < WINDOW // (3 * GROUP) for l, h in zip(low, high)])
    at = iota((WINDOW, LANES), 0).astype(F32).astype(BF16)
    day = iota((LANES, LANES), 0)
    shift = day & 31
    one, zero = jnp.ones((), BF16), jnp.zeros((), BF16)
    acc[...] = jnp.zeros_like(acc)
    tally[...] = jnp.zeros_like(tally)
    firsts[2].wait()
    for q in range(blocks):
        here = slice(q * LANES, (q + 1) * LANES)
        packed = jnp.concatenate(
            [jnp.broadcast_to(bits[w : w + 1, here], (32, LANES)) for w in range(bits.shape[0])],
            axis=0,
        )
        bit = (packed >> shift) & 1
        code = jnp.where(day < limit[q : q + 1], bit, 0) + double_segment[q : q + 1]
        code_ref[here] = code.T
    for copy in loads:
        copy.wait()

    def against(number, start, size):
        return jnp.clip(number - start, -1, size).astype(F32).astype(BF16)

    def spread(lines, q, size):
        return jnp.broadcast_to(lines[q : q + 1], (size, LANES))

    def add_up(windows_of, nearby_of):
        for i in range(steps):
            values, observed_all = [], []
            blocks_here = range(i * per_step, (i + 1) * per_step)
            for q in blocks_here:
                here = slice(q * LANES, (q + 1) * LANES)
                observed = (code_ref[here] & 1).astype(F32)
                value = masked_ref[here] * observed
                masked_ref[here] = value
                values.append(jnp.concatenate(split_two(value), axis=1))
                observed_all.append(observed.astype(BF16))
            values = jnp.concatenate(values, axis=0)
            observed_all = jnp.concatenate(observed_all, axis=0)
            for start in windows_of(i):
                place = against(segment, start, WINDOW)
                hot = jnp.concatenate(
                    [jnp.where(at == spread(place, q, WINDOW), one, zero) for q in blocks_here], axis=1
                )
                acc[pl.ds(start, WINDOW)] += dot(hot, values)
            for start in nearby_of(i):
                place = against(station, start, NEARBY)
                for w, weight in enumerate(weight_of):
                    hot = jnp.concatenate(
                        [
                            jnp.where(
                                at[:NEARBY] == spread(place, q, NEARBY), spread(weight, q, NEARBY), zero
                            )
                            for q in blocks_here
                        ],
                        axis=1,
                    )
                    tally[w, pl.ds(start, NEARBY)] += dot(hot, observed_all)

    @pl.when(close)
    def _():
        add_up(
            lambda i: [pl.multiple_of(low[i] * (3 * GROUP), GROUP)],
            lambda i: [pl.multiple_of(low[i] * GROUP, GROUP)],
        )

    @pl.when(jnp.logical_not(close))
    def _():
        add_up(
            lambda i: range(0, 3 * stations, WINDOW), lambda i: range(0, stations, NEARBY)
        )

    split = (ranges, chunk_count, TILE, stations)
    for k in range(3):
        part = jnp.concatenate(
            [
                acc[(3 * g + k) * GROUP : (3 * g + k + 1) * GROUP]
                for g in range(stations // GROUP)
            ],
            axis=0,
        )
        sums_ref[:, :, k] = (part[:, :LANES] + part[:, LANES:]).T.reshape(split)
    for w in range(len(words)):
        sums_ref[:, :, 3 + w] = tally[w, :stations].T.reshape(split)
    firsts[3].wait()


def remote(src, dst, send, recv, where):
    return pltpu.make_async_remote_copy(
        src_ref=src, dst_ref=dst, send_sem=send, recv_sem=recv,
        device_id=where, device_id_type=pl.DeviceIdType.MESH,
    )


def signal(semaphore, where):
    pl.semaphore_signal(semaphore, inc=1, device_id=where, device_id_type=pl.DeviceIdType.MESH)


def chunk_plan(chips, chunks):
    if chips == 2 and chunks > 1:
        return chunks - 1, chunks + 1
    return chunks, chunks


def pick(index, table):
    value = jnp.int32(table[0])
    for i in range(1, len(table)):
        value = jnp.where(index == i, jnp.int32(table[i]), value)
    return value


def exchange_kernel(
    ranges, owners, major, cell_dev, cell_pad, sums_ref, cells_ref, clim_ref,
    ids, pair, partial, across, got, lhs, started, hot,
    ready, further, pair_send, pair_recv, across_send, across_recv,
    col_send, col_recv, row_send, row_recv, far_send, far_recv, near_send, near_recv,
):
    _, chunks, groups, _, stations = sums_ref.shape
    halves = stations // LANES
    words, base = tally_words(ranges)
    base_bits = base.bit_length() - 1
    width = clim_ref.shape[-1]
    slots = width - stations
    chips, minor = ranges // 2, owners // major
    shared, total_chunks = chunk_plan(chips, chunks)
    id_index = total_chunks
    sta, yr = lax.axis_index("sta"), lax.axis_index("yr")
    chip, core = yr // 2, lax.rem(yr, 2)
    row, place = sta // minor, lax.rem(sta, minor)
    partner = {"yr": chip * 2 + 1 - core}
    chip_at = [lax.rem(chip + k, chips) for k in range(chips)]
    chip_from = [lax.rem(chip + chips - k, chips) for k in range(chips)]
    near_first = [
        sorted(
            (r for r in range(major) if r != mine),
            key=lambda r: (abs(r - mine), r if 2 * mine < major else -r),
        )
        for mine in range(major)
    ]
    relayed = major == 4
    inner = (row == 1) | (row == 2)
    relays = [relayed and 0 < c < id_index for c in range(id_index + 1)]
    turned = [relayed and c > 0 and c != 2 for c in range(id_index)] + [False]
    rows_by = [pick(row, [near_first[m][i] for m in range(major)]) for i in range(major - 1)]

    barrier = pltpu.get_barrier_semaphore()
    beside = [{"sta": row * minor + lax.rem(place + j, minor)} for j in range(1, minor)]
    near_peers = [partner] + [{"yr": c * 2 + core} for c in chip_at[1:]] + beside
    steps_by = [(row > 0, row - 1), (row < major - 1, row + 1)] if relayed else []
    if not relayed:
        near_peers += [{"sta": r * minor + place} for r in rows_by]
    for where in near_peers:
        signal(barrier, where)
    neighbours = pick(row, [1] + [2] * (major - 2) + [1]) if relayed else 0
    for able, to_row in steps_by:
        pl.when(able)(functools.partial(signal, barrier, {"sta": to_row * minor + place}))
    pl.semaphore_wait(barrier, len(near_peers) + neighbours)
    for able, to_row in steps_by:
        pl.when(able)(functools.partial(signal, ready, {"sta": to_row * minor + place}))
    def view(c, owner):
        return got.at[c, owner] if c < id_index else ids.at[owner]

    def send_own(c, which):
        for i in which:
            if relays[c] and i == major - 2:
                pl.when(inner)(col(c, i).start)
            else:
                col(c, i).start()

    def col(c, i):
        block = view(c, sta)
        return remote(
            block, block, col_send.at[c, i], col_recv.at[c, row],
            {"sta": rows_by[i] * minor + place},
        )

    def relay(c):
        block = view(c, rows_by[-1] * minor + place)
        return remote(
            block, block, col_send.at[c, major - 1], col_recv.at[c, rows_by[-1]],
            {"sta": rows_by[0] * minor + place},
        )

    def turn(c, j):
        block = view(c, row * minor + lax.rem(place + minor - j, minor))
        return remote(
            block, block, row_send.at[c, rows_by[0], j - 1], row_recv.at[c, row, j - 1],
            {"sta": rows_by[0] * minor + place},
        )

    def col_in(c, i):
        block = view(c, rows_by[i] * minor + place)
        return remote(
            block, block, col_send.at[c, i], col_recv.at[c, rows_by[i]],
            {"sta": rows_by[i] * minor + place},
        )

    def across_row(c, from_row, j):
        block = view(c, from_row * minor + place)
        return remote(
            block, block, row_send.at[c, from_row, j - 1], row_recv.at[c, from_row, j - 1],
            {"sta": row * minor + lax.rem(place + j, minor)},
        )

    def row_in(c, from_row, j):
        block = view(c, from_row * minor + lax.rem(place + minor - j, minor))
        return remote(
            block, block, row_send.at[c, from_row, j - 1], row_recv.at[c, from_row, j - 1],
            {"sta": row * minor + lax.rem(place + minor - j, minor)},
        )

    pairs = []
    for c in range(chunks):
        for k in [*range(1, chips), 0]:
            copy = remote(
                sums_ref.at[chip_at[k] * 2 + 1 - core, c], pair.at[c, k],
                pair_send.at[c, k], pair_recv.at[c, k], partner,
            )
            copy.start()
            pairs.append(copy)
    ids[sta] = cells_ref[...]
    send_own(id_index, [0])
    for j in range(1, minor):
        across_row(id_index, row, j).start()
    crossing = []
    for c in range(chunks):
        for k in range(1, chips):
            pairs[c * chips + k - 1].wait_recv()
            partial[c, k - 1] = sums_ref[chip_at[k] * 2 + core, c] + pair[c, k]
            copy = remote(
                partial.at[c, k - 1], across.at[c, k - 1],
                across_send.at[c, k - 1], across_recv.at[c, k - 1],
                {"yr": chip_at[k] * 2 + core},
            )
            copy.start()
            crossing.append(copy)

    if total_chunks > chunks:
        c = chunks - 1
        pairs[c * chips + chips - 1].wait_recv()
        partial[chunks, 0] = sums_ref[yr, c] + pair[c, 0]
        copy = remote(
            partial.at[chunks, 0], across.at[chunks, 0],
            across_send.at[chunks, 0], across_recv.at[chunks, 0], {"yr": chip_at[1] * 2 + core},
        )
        copy.start()
        crossing.append(copy)

    def own(c):
        if c == chunks:
            total = partial[c - 1, 0]
        elif c == chunks - 1 and total_chunks > chunks:
            total = partial[chunks, 0]
        else:
            pairs[c * chips + chips - 1].wait_recv()
            total = sums_ref[yr, c] + pair[c, 0]
        for k in range(chips - 1):
            crossing[c * (chips - 1) + k].wait_recv()
            total = total + across[c, k]
        got[c, sta] = total
        send_own(c, range(major - 2, -1, -1))
        for j in range(1, minor):
            across_row(c, row, j).start()

    def pass_on(c, i):
        col_in(c, i).wait_recv()
        if relays[c] and i == major - 2:
            pl.when(inner)(relay(c).start)
        for j in range(1, minor):
            if turned[c] and i == 0:
                row_in(c, row, j).wait_recv()
                turn(c, j).start()
            else:
                across_row(c, rows_by[i], j).start()

    def forward(c):
        for i in range(major - 1):
            pass_on(c, i)

    def side_in(c):
        for j in range(1, minor):
            if not turned[c]:
                row_in(c, row, j).wait_recv()
            for i in range(major - 1):
                row_in(c, rows_by[i], j).wait_recv()

    owner_at = [
        r * minor + lax.rem(place + j, minor) for j in range(minor) for r in [row] + rows_by
    ]

    first = sta * cell_dev
    own_ids = [cells_ref[h : h + 1] for h in range(halves)]

    lane = iota((1, slots), 1)
    target = jnp.concatenate([jnp.where(lane < cell_dev, lane + first, -1)] + own_ids, axis=1)

    def build(low, high):
        for s in range(low, high):
            column = ids[owner_at[s]].T
            for h in range(halves):
                at = s * stations + h * LANES
                hot[at : at + LANES] = one_where(column[:, h : h + 1] == target)

    def add_shards(c, low, high):
        for s in range(low, high):
            owner = owner_at[s]
            sums = [got[c, owner, k] for k in range(3)]
            high_part = [v.astype(BF16).astype(F32) for v in sums]
            low_part = [v - h for v, h in zip(sums, high_part)]
            tallies = [None] * 3
            for w, held in enumerate(words):
                word = got[c, owner, 3 + w].astype(I32)
                for p, k in enumerate(held):
                    tallies[k] = ((word >> (p * base_bits)) & (base - 1)).astype(F32)
            parts = high_part + low_part + tallies
            if base > 256:
                rounded = [t.astype(BF16).astype(F32) for t in tallies]
                parts = high_part + low_part + rounded + [t - r for t, r in zip(tallies, rounded)]
            if len(parts) % 2:
                parts.append(jnp.zeros_like(parts[0]))
            lhs[:, s * stations : (s + 1) * stations] = jnp.concatenate(parts, axis=0).astype(BF16)
        here = slice(low * stations, high * stations)
        return dot(lhs[:, here], hot[here])

    def cells_start(c):
        started[...] = add_shards(c, 0, major)

    def cells(c):
        side_in(c)
        total = started[...] + add_shards(c, major, owners) if minor > 1 else started[...]
        step = 3 * TILE
        tally = total[2 * step : 3 * step]
        if base > 256:
            tally = tally + total[3 * step : 4 * step]
        clim = (total[:step] + total[step : 2 * step]) / jnp.maximum(tally, 1.0)
        clim = clim.reshape(3, TILE, width)
        if c == chunks:
            clim_ref[chip_at[1] * 2 + core, c - 1] = clim
            near(c - 1, 1).start()
            return
        clim_ref[yr, c] = clim
        if c < shared:
            for k in range(1, chips):
                far(c, k).start()
        near(c, 0).start()

    def far(c, k):
        block = clim_ref.at[yr, c]
        return remote(
            block, block, far_send.at[c, k - 1], far_recv.at[c, k - 1],
            {"yr": chip_at[k] * 2 + core},
        )

    def near(c, k):
        block = clim_ref.at[chip_from[k] * 2 + core, c]
        return remote(block, block, near_send.at[c, k], near_recv.at[c, k], partner)

    def hand_on(c):
        for k in range(1, chips):
            far(c, k).wait_recv()
            near(c, k).start()

    if relayed:
        pl.semaphore_wait(ready, neighbours)
        for able, to_row in steps_by:
            pl.when(able)(functools.partial(signal, further, {"sta": to_row * minor + place}))
        pl.semaphore_wait(further, neighbours)
    send_own(id_index, range(1, major - 1))
    last = major - 2
    for c in range(min(chunks, 2)):
        own(c)
        if c < last:
            pass_on(id_index, c)
    for i in range(min(chunks, 2, last), last + 1):
        pass_on(id_index, i)
    for i in range(last):
        pass_on(0, i)
    if chunks > 2:
        own(2)
    build(0, last + 1)
    pass_on(0, last)
    for c in range(3, total_chunks):
        own(c)
    build(last + 1, major)
    cells_start(0)
    if chunks > 1:
        for i in range(major - 2):
            pass_on(1, i)
    side_in(id_index)
    build(major, owners)
    if chunks > 1:
        pass_on(1, major - 2)
    handed = 0
    for c in range(total_chunks):
        if c > 0 and c + 1 < total_chunks:
            forward(c + 1)
        if c >= 3 and handed < shared:
            hand_on(handed)
            handed += 1
        cells(c)
        if c + 1 < total_chunks:
            cells_start(c + 1)
    for c in range(handed, shared):
        hand_on(c)
    for c in range(chunks):
        for k in range(chips):
            near(c, k).wait()
        if c >= shared:
            continue
        for k in range(1, chips):
            far(c, k).wait_send()
    for c in range(id_index + 1):
        for i in range(major - 1):
            if relays[c] and i == major - 2:
                pl.when(inner)(col(c, i).wait_send)
                pl.when(inner)(relay(c).wait_send)
            else:
                col(c, i).wait_send()
        for j in range(1, minor):
            across_row(c, row, j).wait_send()
            for i in range(major - 1):
                across_row(c, rows_by[i], j).wait_send()
    for copy in pairs + crossing:
        copy.wait_send()


def anomaly_kernel(
    ranges, cell_dev, cell_pad, rows, masked_ref, code_ref, clim_ref,
    out_hbm, climatology_hbm, table, clim_buf, out_buf, clim_sem, out_sem,
):
    block_total, days = masked_ref.shape
    stations = clim_ref.shape[-1] - cell_pad
    steps = block_total // rows
    low, high = [], []
    for i in range(steps):
        ends = [code_ref[at : at + TILE] for at in (i * rows, (i + 1) * rows - TILE)]
        low.append((jnp.min(ends[0]) >> 1) // (3 * GROUP))
        high.append((jnp.max(ends[1]) >> 1) // (3 * GROUP))
    close = functools.reduce(jnp.logical_and, [h - l < WINDOW // (3 * GROUP) for l, h in zip(low, high)])
    for k in range(3):
        part = clim_ref[:, :, k, :, cell_pad:].reshape(days, stations).T
        both = jnp.concatenate(split_two(part), axis=1)
        for g in range(stations // GROUP):
            at = (3 * g + k) * GROUP
            table[at : at + GROUP] = both[g * GROUP : (g + 1) * GROUP]
    table[3 * stations :] = jnp.zeros((table.shape[0] - 3 * stations, 2 * days), BF16)
    clim_copy = pltpu.make_async_copy(clim_buf, climatology_hbm, clim_sem.at[0])
    copies = [
        pltpu.make_async_copy(
            out_buf.at[i * rows : (i + 1) * rows], out_hbm.at[i * rows : (i + 1) * rows], out_sem.at[i]
        )
        for i in range(steps)
    ]
    for j in range(cell_pad // LANES):
        for k in range(3):
            part = clim_ref[:, :, k, :, j * LANES : (j + 1) * LANES].reshape(days, LANES)
            last = min((j + 1) * LANES, cell_dev)
            clim_buf[j * LANES : last, k * days : (k + 1) * days] = part.T[: last - j * LANES]
    clim_copy.start()

    def subtract(windows_of):
        lane = iota((rows, LANES), 1)
        for i in range(steps):
            here = slice(i * rows, (i + 1) * rows)
            code = code_ref[here]
            segment = code >> 1
            found = None
            for start in windows_of(i):
                place = segment - start
                hot = jnp.concatenate(
                    [one_where(place == lane + j) for j in range(0, WINDOW, LANES)], axis=1
                )
                part = dot(hot, table[pl.ds(start, WINDOW)])
                found = part if found is None else found + part
            clim = found[:, :days] + found[:, days:]
            out_buf[here] = masked_ref[here] - (code & 1).astype(F32) * clim
            copies[i].start()

    @pl.when(close)
    def _():
        subtract(lambda i: [pl.multiple_of(low[i] * (3 * GROUP), GROUP)])

    @pl.when(jnp.logical_not(close))
    def _():
        subtract(lambda i: range(0, 3 * stations, WINDOW))

    for copy in [clim_copy] + copies:
        copy.wait()


def per_device(temps, day_bits, block_offset, block_counts, station_cell):
    owners, ranges = lax.axis_size("sta"), lax.axis_size("yr")
    stations = station_cell.shape[0]
    block_total, days = temps.shape
    cell_dev = CELLS // owners
    cell_pad = round_up(cell_dev, LANES)
    width = cell_pad + stations
    words, base = tally_words(ranges)
    groups = 3 + len(words)
    chunks = days // ranges // TILE
    rows = 1024 if block_total % 1024 == 0 else block_total
    major = 4 if owners % 4 == 0 else owners
    minor, chips = owners // major, ranges // 2
    dma = pltpu.SemaphoreType.DMA
    whole = pl.BlockSpec(memory_space=VMEM)
    hbm = pl.BlockSpec(memory_space=pltpu.HBM)

    inputs = [
        pltpu.with_memory_space_constraint(array, pltpu.HBM)
        for array in (
            temps, day_bits, block_offset.reshape(block_total // LANES, LANES), block_counts,
            station_cell.reshape(stations // LANES, LANES),
        )
    ]
    sums, masked, code, cells = pl.pallas_call(
        functools.partial(sums_kernel, ranges, rows),
        in_specs=[hbm] * 5,
        out_specs=[whole] * 4,
        out_shape=[
            jax.ShapeDtypeStruct((ranges, chunks, groups, TILE, stations), F32),
            jax.ShapeDtypeStruct((block_total, days), F32),
            jax.ShapeDtypeStruct((block_total, days), I32),
            jax.ShapeDtypeStruct((TILE, LANES), I32),
        ],
        scratch_shapes=[
            VMEM((day_bits.shape[0], block_total), I32),
            VMEM((block_total // LANES, LANES), I32),
            VMEM((1, stations), I32),
            VMEM((round_up(3 * stations, WINDOW) + WINDOW, 2 * days), F32),
            VMEM((len(words), stations + 2 * NEARBY, days), F32),
            dma((4,)), dma((block_total // rows,)),
        ],
        compiler_params=pltpu.CompilerParams(vmem_limit_bytes=40 * 1024 * 1024),
    )(*inputs)

    block = (groups, TILE, stations)
    parts = 3 * 3 if base <= 256 else 3 * 4
    total_chunks = chunk_plan(chips, chunks)[1]
    crossings, sides = max(chips - 1, 1), max(minor - 1, 1)
    clim = pl.pallas_call(
        functools.partial(exchange_kernel, ranges, owners, major, cell_dev, cell_pad),
        in_specs=[whole] * 2,
        out_specs=whole,
        out_shape=jax.ShapeDtypeStruct((ranges, chunks, 3, TILE, width), F32),
        scratch_shapes=[
            VMEM((owners, TILE, LANES), I32),
            VMEM((chunks, chips) + block, F32),
            VMEM((total_chunks, crossings) + block, F32),
            VMEM((total_chunks, crossings) + block, F32),
            VMEM((total_chunks, owners) + block, F32),
            VMEM((round_up(parts * TILE, 16), owners * stations), BF16),
            VMEM((round_up(parts * TILE, 16), width), F32),
            VMEM((owners * stations, width), BF16),
            pltpu.SemaphoreType.REGULAR, pltpu.SemaphoreType.REGULAR,
            dma((chunks, chips)), dma((chunks, chips)),
            dma((total_chunks, crossings)), dma((total_chunks, crossings)),
            dma((total_chunks + 1, major)), dma((total_chunks + 1, major)),
            dma((total_chunks + 1, major, sides)), dma((total_chunks + 1, major, sides)),
            dma((chunks, crossings)), dma((chunks, crossings)),
            dma((chunks, chips)), dma((chunks, chips)),
        ],
        compiler_params=pltpu.CompilerParams(
            collective_id=0, has_side_effects=True, vmem_limit_bytes=40 * 1024 * 1024
        ),
    )(sums, cells)

    rows = 512 if block_total % 512 == 0 else block_total
    return pl.pallas_call(
        functools.partial(anomaly_kernel, ranges, cell_dev, cell_pad, rows),
        in_specs=[whole] * 3,
        out_specs=[hbm] * 2,
        out_shape=[
            jax.ShapeDtypeStruct((block_total, days), F32),
            jax.ShapeDtypeStruct((cell_dev, 3 * days), F32),
        ],
        scratch_shapes=[
            VMEM((round_up(3 * stations, WINDOW) + WINDOW, 2 * days), BF16),
            VMEM((cell_dev, 3 * days), F32),
            VMEM((block_total, days), F32),
            dma((1,)), dma((block_total // rows,)),
        ],
        compiler_params=pltpu.CompilerParams(vmem_limit_bytes=40 * 1024 * 1024),
    )(masked, code, clim)


def solution(mesh):
    in_specs = (
        P(("sta", "yr"), None),
        P(None, ("sta", "yr")),
        P(("sta", "yr")),
        P("yr", "sta"),
        P("sta"),
    )
    out_specs = (P(("sta", "yr"), None), P("sta", None))

    def run(*args):
        return tuple(per_device(*args))

    return jax.shard_map(
        run, mesh=mesh, in_specs=in_specs, out_specs=out_specs, check_vma=False
    )
```

```python
import functools

import jax
import jax.numpy as jnp
from jax import lax
from jax.experimental import pallas as pl
from jax.experimental.pallas import tpu as pltpu
from jax.sharding import PartitionSpec as P

CELLS = 10368
CALENDAR = 365
MOST_BLOCKS = 48
LANES = 128
TILE = 8
GROUP = 16
WINDOW = 256
NEARBY = 96
F32 = jnp.float32
BF16 = jnp.bfloat16
I32 = jnp.int32
VMEM = pltpu.VMEM


def round_up(value, step):
    return (value + step - 1) // step * step


def tally_words(ranges):
    if ranges * MOST_BLOCKS < 256:
        return [(0, 1, 2)], 256
    return [(0, 1), (2,)], 4096


def iota(shape, dim):
    return lax.broadcasted_iota(I32, shape, dim)


def one_where(mask):
    return jnp.where(mask, 1.0, 0.0).astype(BF16)


def dot(a, b, dims=((1,), (0,))):
    return lax.dot_general(a, b, (dims, ((), ())), preferred_element_type=F32)


def split_two(value):
    high = value.astype(BF16)
    return high, (value - high.astype(F32)).astype(BF16)


def row_stations(counts, blocks):
    stations = counts.shape[1]
    spread = jnp.broadcast_to(counts.astype(F32), (LANES, stations)).astype(BF16)
    square = (stations, stations)
    ends = dot(one_where(iota(square, 1) <= iota(square, 0)), spread, ((1,), (1,))).astype(I32)
    lane = iota((stations, LANES), 1)
    ending = dot(one_where((ends >> 7) == lane), one_where((ends & 127) == lane), ((0,), (0,)))
    ending = ending.astype(BF16)
    tile = (LANES, LANES)
    within = dot(ending, one_where(iota(tile, 0) <= iota(tile, 1)))
    totals = dot(ending, jnp.ones(tile, BF16)).astype(BF16)
    before = dot(one_where(iota(tile, 1) < iota(tile, 0)), totals)
    return (within + before)[:blocks]


def sums_kernel(
    ranges, rows, temps_hbm, bits_hbm, offs_hbm, counts_hbm, cell_hbm,
    sums_ref, masked_ref, code_ref, cells_ref, bits, offs, counts, acc, tally, small, large,
):
    block_total = masked_ref.shape[0]
    blocks, stations = offs.shape[0], counts.shape[1]
    words, base = tally_words(ranges)
    chunk_count = sums_ref.shape[1]
    firsts = [
        pltpu.make_async_copy(counts_hbm, counts, small.at[0]),
        pltpu.make_async_copy(offs_hbm, offs, small.at[1]),
        pltpu.make_async_copy(bits_hbm, bits, small.at[2]),
        pltpu.make_async_copy(cell_hbm, cells_ref.at[0 : cell_hbm.shape[0]], small.at[3]),
    ]
    steps = block_total // rows
    loads = [
        pltpu.make_async_copy(
            temps_hbm.at[i * rows : (i + 1) * rows], masked_ref.at[i * rows : (i + 1) * rows],
            large.at[i],
        )
        for i in range(steps)
    ]
    for copy in firsts + loads:
        copy.start()
    firsts[0].wait()
    station = row_stations(counts[...], blocks)
    firsts[1].wait()
    offsets = offs[...]
    third = offsets - 3 * ((offsets * 21846) >> 16)
    station = station.astype(I32)
    segment = (station // GROUP) * (3 * GROUP) + third * GROUP + station % GROUP
    double_segment = 2 * segment
    limit = CALENDAR - LANES * third
    weight_of = []
    for held in words:
        weight = jnp.zeros(third.shape, F32)
        for place, k in enumerate(held):
            weight = jnp.where(third == k, float(base**place), weight)
        weight_of.append(weight.astype(BF16))
    group = station // GROUP
    per_step = rows // LANES
    low = [jnp.min(group[i * per_step : (i + 1) * per_step]) for i in range(steps)]
    high = [jnp.max(group[i * per_step : (i + 1) * per_step]) for i in range(steps)]
    close = functools.reduce(jnp.logical_and, [h - l < WINDOW // (3 * GROUP) for l, h in zip(low, high)])
    at = iota((WINDOW, LANES), 0).astype(F32).astype(BF16)
    day = iota((LANES, LANES), 0)
    shift = day & 31
    one, zero = jnp.ones((), BF16), jnp.zeros((), BF16)
    acc[...] = jnp.zeros_like(acc)
    tally[...] = jnp.zeros_like(tally)
    firsts[2].wait()
    for q in range(blocks):
        here = slice(q * LANES, (q + 1) * LANES)
        packed = jnp.concatenate(
            [jnp.broadcast_to(bits[w : w + 1, here], (32, LANES)) for w in range(bits.shape[0])],
            axis=0,
        )
        bit = (packed >> shift) & 1
        code = jnp.where(day < limit[q : q + 1], bit, 0) + double_segment[q : q + 1]
        code_ref[here] = code.T
    for copy in loads:
        copy.wait()

    def against(number, start, size):
        return jnp.clip(number - start, -1, size).astype(F32).astype(BF16)

    def spread(lines, q, size):
        return jnp.broadcast_to(lines[q : q + 1], (size, LANES))

    def add_up(windows_of, nearby_of):
        for i in range(steps):
            values, observed_all = [], []
            blocks_here = range(i * per_step, (i + 1) * per_step)
            for q in blocks_here:
                here = slice(q * LANES, (q + 1) * LANES)
                observed = (code_ref[here] & 1).astype(F32)
                value = masked_ref[here] * observed
                masked_ref[here] = value
                values.append(jnp.concatenate(split_two(value), axis=1))
                observed_all.append(observed.astype(BF16))
            values = jnp.concatenate(values, axis=0)
            observed_all = jnp.concatenate(observed_all, axis=0)
            for start in windows_of(i):
                place = against(segment, start, WINDOW)
                hot = jnp.concatenate(
                    [jnp.where(at == spread(place, q, WINDOW), one, zero) for q in blocks_here], axis=1
                )
                acc[pl.ds(start, WINDOW)] += dot(hot, values)
            for start in nearby_of(i):
                place = against(station, start, NEARBY)
                for w, weight in enumerate(weight_of):
                    hot = jnp.concatenate(
                        [
                            jnp.where(
                                at[:NEARBY] == spread(place, q, NEARBY), spread(weight, q, NEARBY), zero
                            )
                            for q in blocks_here
                        ],
                        axis=1,
                    )
                    tally[w, pl.ds(start, NEARBY)] += dot(hot, observed_all)

    @pl.when(close)
    def _():
        add_up(
            lambda i: [pl.multiple_of(low[i] * (3 * GROUP), GROUP)],
            lambda i: [pl.multiple_of(low[i] * GROUP, GROUP)],
        )

    @pl.when(jnp.logical_not(close))
    def _():
        add_up(
            lambda i: range(0, 3 * stations, WINDOW), lambda i: range(0, stations, NEARBY)
        )

    split = (ranges, chunk_count, TILE, stations)
    for k in range(3):
        part = jnp.concatenate(
            [
                acc[(3 * g + k) * GROUP : (3 * g + k + 1) * GROUP]
                for g in range(stations // GROUP)
            ],
            axis=0,
        )
        sums_ref[:, :, k] = (part[:, :LANES] + part[:, LANES:]).T.reshape(split)
    for w in range(len(words)):
        sums_ref[:, :, 3 + w] = tally[w, :stations].T.reshape(split)
    firsts[3].wait()


def remote(src, dst, send, recv, where):
    return pltpu.make_async_remote_copy(
        src_ref=src, dst_ref=dst, send_sem=send, recv_sem=recv,
        device_id=where, device_id_type=pl.DeviceIdType.MESH,
    )


def signal(semaphore, where):
    pl.semaphore_signal(semaphore, inc=1, device_id=where, device_id_type=pl.DeviceIdType.MESH)


def chunk_plan(chips, chunks):
    if chips == 2 and chunks > 1:
        return chunks - 1, chunks + 1
    return chunks, chunks


def pick(index, table):
    value = jnp.int32(table[0])
    for i in range(1, len(table)):
        value = jnp.where(index == i, jnp.int32(table[i]), value)
    return value


def exchange_kernel(
    ranges, owners, major, cell_dev, cell_pad, sums_ref, cells_ref, clim_ref,
    ids, pair, partial, across, got, lhs, started, hot,
    ready, further, pair_send, pair_recv, across_send, across_recv,
    col_send, col_recv, row_send, row_recv, far_send, far_recv, near_send, near_recv,
):
    _, chunks, groups, _, stations = sums_ref.shape
    halves = stations // LANES
    words, base = tally_words(ranges)
    base_bits = base.bit_length() - 1
    width = clim_ref.shape[-1]
    slots = width - stations
    chips, minor = ranges // 2, owners // major
    shared, total_chunks = chunk_plan(chips, chunks)
    id_index = total_chunks
    sta, yr = lax.axis_index("sta"), lax.axis_index("yr")
    chip, core = yr // 2, lax.rem(yr, 2)
    row, place = sta // minor, lax.rem(sta, minor)
    partner = {"yr": chip * 2 + 1 - core}
    chip_at = [lax.rem(chip + k, chips) for k in range(chips)]
    chip_from = [lax.rem(chip + chips - k, chips) for k in range(chips)]
    near_first = [
        sorted(
            (r for r in range(major) if r != mine),
            key=lambda r: (abs(r - mine), r if 2 * mine < major else -r),
        )
        for mine in range(major)
    ]
    relayed = major == 4
    inner = (row == 1) | (row == 2)
    relays = [relayed and 0 < c < id_index for c in range(id_index + 1)]
    turned = [relayed and c > 0 and c != 2 for c in range(id_index)] + [False]
    rows_by = [pick(row, [near_first[m][i] for m in range(major)]) for i in range(major - 1)]

    barrier = pltpu.get_barrier_semaphore()
    beside = [{"sta": row * minor + lax.rem(place + j, minor)} for j in range(1, minor)]
    near_peers = [partner] + [{"yr": c * 2 + core} for c in chip_at[1:]] + beside
    steps_by = [(row > 0, row - 1), (row < major - 1, row + 1)] if relayed else []
    if not relayed:
        near_peers += [{"sta": r * minor + place} for r in rows_by]
    for where in near_peers:
        signal(barrier, where)
    neighbours = pick(row, [1] + [2] * (major - 2) + [1]) if relayed else 0
    for able, to_row in steps_by:
        pl.when(able)(functools.partial(signal, barrier, {"sta": to_row * minor + place}))
    pl.semaphore_wait(barrier, len(near_peers) + neighbours)
    for able, to_row in steps_by:
        pl.when(able)(functools.partial(signal, ready, {"sta": to_row * minor + place}))
    def view(c, owner):
        return got.at[c, owner] if c < id_index else ids.at[owner]

    def send_own(c, which):
        for i in which:
            if relays[c] and i == major - 2:
                pl.when(inner)(col(c, i).start)
            else:
                col(c, i).start()

    def col(c, i):
        block = view(c, sta)
        return remote(
            block, block, col_send.at[c, i], col_recv.at[c, row],
            {"sta": rows_by[i] * minor + place},
        )

    def relay(c):
        block = view(c, rows_by[-1] * minor + place)
        return remote(
            block, block, col_send.at[c, major - 1], col_recv.at[c, rows_by[-1]],
            {"sta": rows_by[0] * minor + place},
        )

    def turn(c, j):
        block = view(c, row * minor + lax.rem(place + minor - j, minor))
        return remote(
            block, block, row_send.at[c, rows_by[0], j - 1], row_recv.at[c, row, j - 1],
            {"sta": rows_by[0] * minor + place},
        )

    def col_in(c, i):
        block = view(c, rows_by[i] * minor + place)
        return remote(
            block, block, col_send.at[c, i], col_recv.at[c, rows_by[i]],
            {"sta": rows_by[i] * minor + place},
        )

    def across_row(c, from_row, j):
        block = view(c, from_row * minor + place)
        return remote(
            block, block, row_send.at[c, from_row, j - 1], row_recv.at[c, from_row, j - 1],
            {"sta": row * minor + lax.rem(place + j, minor)},
        )

    def row_in(c, from_row, j):
        block = view(c, from_row * minor + lax.rem(place + minor - j, minor))
        return remote(
            block, block, row_send.at[c, from_row, j - 1], row_recv.at[c, from_row, j - 1],
            {"sta": row * minor + lax.rem(place + minor - j, minor)},
        )

    pairs = []
    for c in range(chunks):
        for k in [*range(1, chips), 0]:
            copy = remote(
                sums_ref.at[chip_at[k] * 2 + 1 - core, c], pair.at[c, k],
                pair_send.at[c, k], pair_recv.at[c, k], partner,
            )
            copy.start()
            pairs.append(copy)
    ids[sta] = cells_ref[...]
    send_own(id_index, [0])
    for j in range(1, minor):
        across_row(id_index, row, j).start()
    crossing = []
    for c in range(chunks):
        for k in range(1, chips):
            pairs[c * chips + k - 1].wait_recv()
            partial[c, k - 1] = sums_ref[chip_at[k] * 2 + core, c] + pair[c, k]
            copy = remote(
                partial.at[c, k - 1], across.at[c, k - 1],
                across_send.at[c, k - 1], across_recv.at[c, k - 1],
                {"yr": chip_at[k] * 2 + core},
            )
            copy.start()
            crossing.append(copy)

    if total_chunks > chunks:
        c = chunks - 1
        pairs[c * chips + chips - 1].wait_recv()
        partial[chunks, 0] = sums_ref[yr, c] + pair[c, 0]
        copy = remote(
            partial.at[chunks, 0], across.at[chunks, 0],
            across_send.at[chunks, 0], across_recv.at[chunks, 0], {"yr": chip_at[1] * 2 + core},
        )
        copy.start()
        crossing.append(copy)

    def own(c):
        if c == chunks:
            total = partial[c - 1, 0]
        elif c == chunks - 1 and total_chunks > chunks:
            total = partial[chunks, 0]
        else:
            pairs[c * chips + chips - 1].wait_recv()
            total = sums_ref[yr, c] + pair[c, 0]
        for k in range(chips - 1):
            crossing[c * (chips - 1) + k].wait_recv()
            total = total + across[c, k]
        got[c, sta] = total
        send_own(c, range(major - 2, -1, -1))
        for j in range(1, minor):
            across_row(c, row, j).start()

    def pass_on(c, i):
        col_in(c, i).wait_recv()
        if relays[c] and i == major - 2:
            pl.when(inner)(relay(c).start)
        for j in range(1, minor):
            if turned[c] and i == 0:
                row_in(c, row, j).wait_recv()
                turn(c, j).start()
            else:
                across_row(c, rows_by[i], j).start()

    def forward(c):
        for i in range(major - 1):
            pass_on(c, i)

    def side_in(c):
        for j in range(1, minor):
            if not turned[c]:
                row_in(c, row, j).wait_recv()
            for i in range(major - 1):
                row_in(c, rows_by[i], j).wait_recv()

    owner_at = [
        r * minor + lax.rem(place + j, minor) for j in range(minor) for r in [row] + rows_by
    ]

    first = sta * cell_dev
    own_ids = [cells_ref[h : h + 1] for h in range(halves)]

    lane = iota((1, slots), 1)
    target = jnp.concatenate([jnp.where(lane < cell_dev, lane + first, -1)] + own_ids, axis=1)

    def build(low, high):
        for s in range(low, high):
            column = ids[owner_at[s]].T
            for h in range(halves):
                at = s * stations + h * LANES
                hot[at : at + LANES] = one_where(column[:, h : h + 1] == target)

    def add_shards(c, low, high):
        for s in range(low, high):
            owner = owner_at[s]
            sums = [got[c, owner, k] for k in range(3)]
            high_part = [v.astype(BF16).astype(F32) for v in sums]
            low_part = [v - h for v, h in zip(sums, high_part)]
            tallies = [None] * 3
            for w, held in enumerate(words):
                word = got[c, owner, 3 + w].astype(I32)
                for p, k in enumerate(held):
                    tallies[k] = ((word >> (p * base_bits)) & (base - 1)).astype(F32)
            parts = high_part + low_part + tallies
            if base > 256:
                rounded = [t.astype(BF16).astype(F32) for t in tallies]
                parts = high_part + low_part + rounded + [t - r for t, r in zip(tallies, rounded)]
            if len(parts) % 2:
                parts.append(jnp.zeros_like(parts[0]))
            lhs[:, s * stations : (s + 1) * stations] = jnp.concatenate(parts, axis=0).astype(BF16)
        here = slice(low * stations, high * stations)
        return dot(lhs[:, here], hot[here])

    def cells_start(c):
        started[...] = add_shards(c, 0, major)

    def cells(c):
        side_in(c)
        total = started[...] + add_shards(c, major, owners) if minor > 1 else started[...]
        step = 3 * TILE
        tally = total[2 * step : 3 * step]
        if base > 256:
            tally = tally + total[3 * step : 4 * step]
        clim = (total[:step] + total[step : 2 * step]) / jnp.maximum(tally, 1.0)
        clim = clim.reshape(3, TILE, width)
        if c == chunks:
            clim_ref[chip_at[1] * 2 + core, c - 1] = clim
            near(c - 1, 1).start()
            return
        clim_ref[yr, c] = clim
        if c < shared:
            for k in range(1, chips):
                far(c, k).start()
        near(c, 0).start()

    def far(c, k):
        block = clim_ref.at[yr, c]
        return remote(
            block, block, far_send.at[c, k - 1], far_recv.at[c, k - 1],
            {"yr": chip_at[k] * 2 + core},
        )

    def near(c, k):
        block = clim_ref.at[chip_from[k] * 2 + core, c]
        return remote(block, block, near_send.at[c, k], near_recv.at[c, k], partner)

    def hand_on(c):
        for k in range(1, chips):
            far(c, k).wait_recv()
            near(c, k).start()

    if relayed:
        pl.semaphore_wait(ready, neighbours)
        for able, to_row in steps_by:
            pl.when(able)(functools.partial(signal, further, {"sta": to_row * minor + place}))
        pl.semaphore_wait(further, neighbours)
    send_own(id_index, range(1, major - 1))
    last = major - 2
    for c in range(min(chunks, 2)):
        own(c)
        if c < last:
            pass_on(id_index, c)
    for i in range(min(chunks, 2, last), last + 1):
        pass_on(id_index, i)
    for i in range(last):
        pass_on(0, i)
    if chunks > 2:
        own(2)
    build(0, last + 1)
    pass_on(0, last)
    for c in range(3, chunks):
        own(c)
    build(last + 1, major)
    cells_start(0)
    if chunks > 1:
        for i in range(major - 2):
            pass_on(1, i)
    side_in(id_index)
    build(major, owners)
    if chunks > 1:
        pass_on(1, major - 2)
    handed = 0
    for c in range(total_chunks):
        if c > 0 and c + 1 < total_chunks:
            forward(c + 1)
        if c >= 3 and handed < shared:
            hand_on(handed)
            handed += 1
        cells(c)
        if c + 1 < total_chunks:
            cells_start(c + 1)
        if c == 0 and total_chunks > chunks:
            own(chunks)
    for c in range(handed, shared):
        hand_on(c)
    for c in range(chunks):
        for k in range(chips):
            near(c, k).wait()
        if c >= shared:
            continue
        for k in range(1, chips):
            far(c, k).wait_send()
    for c in range(id_index + 1):
        for i in range(major - 1):
            if relays[c] and i == major - 2:
                pl.when(inner)(col(c, i).wait_send)
                pl.when(inner)(relay(c).wait_send)
            else:
                col(c, i).wait_send()
        for j in range(1, minor):
            across_row(c, row, j).wait_send()
            for i in range(major - 1):
                across_row(c, rows_by[i], j).wait_send()
    for copy in pairs + crossing:
        copy.wait_send()


def anomaly_kernel(
    ranges, cell_dev, cell_pad, rows, masked_ref, code_ref, clim_ref,
    out_hbm, climatology_hbm, table, clim_buf, out_buf, clim_sem, out_sem,
):
    block_total, days = masked_ref.shape
    stations = clim_ref.shape[-1] - cell_pad
    steps = block_total // rows
    low, high = [], []
    for i in range(steps):
        ends = [code_ref[at : at + TILE] for at in (i * rows, (i + 1) * rows - TILE)]
        low.append((jnp.min(ends[0]) >> 1) // (3 * GROUP))
        high.append((jnp.max(ends[1]) >> 1) // (3 * GROUP))
    close = functools.reduce(jnp.logical_and, [h - l < WINDOW // (3 * GROUP) for l, h in zip(low, high)])
    for k in range(3):
        part = clim_ref[:, :, k, :, cell_pad:].reshape(days, stations).T
        both = jnp.concatenate(split_two(part), axis=1)
        for g in range(stations // GROUP):
            at = (3 * g + k) * GROUP
            table[at : at + GROUP] = both[g * GROUP : (g + 1) * GROUP]
    table[3 * stations :] = jnp.zeros((table.shape[0] - 3 * stations, 2 * days), BF16)
    clim_copy = pltpu.make_async_copy(clim_buf, climatology_hbm, clim_sem.at[0])
    copies = [
        pltpu.make_async_copy(
            out_buf.at[i * rows : (i + 1) * rows], out_hbm.at[i * rows : (i + 1) * rows], out_sem.at[i]
        )
        for i in range(steps)
    ]
    for j in range(cell_pad // LANES):
        for k in range(3):
            part = clim_ref[:, :, k, :, j * LANES : (j + 1) * LANES].reshape(days, LANES)
            last = min((j + 1) * LANES, cell_dev)
            clim_buf[j * LANES : last, k * days : (k + 1) * days] = part.T[: last - j * LANES]
    clim_copy.start()

    def subtract(windows_of):
        lane = iota((rows, LANES), 1)
        for i in range(steps):
            here = slice(i * rows, (i + 1) * rows)
            code = code_ref[here]
            segment = code >> 1
            found = None
            for start in windows_of(i):
                place = segment - start
                hot = jnp.concatenate(
                    [one_where(place == lane + j) for j in range(0, WINDOW, LANES)], axis=1
                )
                part = dot(hot, table[pl.ds(start, WINDOW)])
                found = part if found is None else found + part
            clim = found[:, :days] + found[:, days:]
            out_buf[here] = masked_ref[here] - (code & 1).astype(F32) * clim
            copies[i].start()

    @pl.when(close)
    def _():
        subtract(lambda i: [pl.multiple_of(low[i] * (3 * GROUP), GROUP)])

    @pl.when(jnp.logical_not(close))
    def _():
        subtract(lambda i: range(0, 3 * stations, WINDOW))

    for copy in [clim_copy] + copies:
        copy.wait()


def per_device(temps, day_bits, block_offset, block_counts, station_cell):
    owners, ranges = lax.axis_size("sta"), lax.axis_size("yr")
    stations = station_cell.shape[0]
    block_total, days = temps.shape
    cell_dev = CELLS // owners
    cell_pad = round_up(cell_dev, LANES)
    width = cell_pad + stations
    words, base = tally_words(ranges)
    groups = 3 + len(words)
    chunks = days // ranges // TILE
    rows = 1024 if block_total % 1024 == 0 else block_total
    major = 4 if owners % 4 == 0 else owners
    minor, chips = owners // major, ranges // 2
    dma = pltpu.SemaphoreType.DMA
    whole = pl.BlockSpec(memory_space=VMEM)
    hbm = pl.BlockSpec(memory_space=pltpu.HBM)

    inputs = [
        pltpu.with_memory_space_constraint(array, pltpu.HBM)
        for array in (
            temps, day_bits, block_offset.reshape(block_total // LANES, LANES), block_counts,
            station_cell.reshape(stations // LANES, LANES),
        )
    ]
    sums, masked, code, cells = pl.pallas_call(
        functools.partial(sums_kernel, ranges, rows),
        in_specs=[hbm] * 5,
        out_specs=[whole] * 4,
        out_shape=[
            jax.ShapeDtypeStruct((ranges, chunks, groups, TILE, stations), F32),
            jax.ShapeDtypeStruct((block_total, days), F32),
            jax.ShapeDtypeStruct((block_total, days), I32),
            jax.ShapeDtypeStruct((TILE, LANES), I32),
        ],
        scratch_shapes=[
            VMEM((day_bits.shape[0], block_total), I32),
            VMEM((block_total // LANES, LANES), I32),
            VMEM((1, stations), I32),
            VMEM((round_up(3 * stations, WINDOW) + WINDOW, 2 * days), F32),
            VMEM((len(words), stations + 2 * NEARBY, days), F32),
            dma((4,)), dma((block_total // rows,)),
        ],
        compiler_params=pltpu.CompilerParams(vmem_limit_bytes=40 * 1024 * 1024),
    )(*inputs)

    block = (groups, TILE, stations)
    parts = 3 * 3 if base <= 256 else 3 * 4
    total_chunks = chunk_plan(chips, chunks)[1]
    crossings, sides = max(chips - 1, 1), max(minor - 1, 1)
    clim = pl.pallas_call(
        functools.partial(exchange_kernel, ranges, owners, major, cell_dev, cell_pad),
        in_specs=[whole] * 2,
        out_specs=whole,
        out_shape=jax.ShapeDtypeStruct((ranges, chunks, 3, TILE, width), F32),
        scratch_shapes=[
            VMEM((owners, TILE, LANES), I32),
            VMEM((chunks, chips) + block, F32),
            VMEM((total_chunks, crossings) + block, F32),
            VMEM((total_chunks, crossings) + block, F32),
            VMEM((total_chunks, owners) + block, F32),
            VMEM((round_up(parts * TILE, 16), owners * stations), BF16),
            VMEM((round_up(parts * TILE, 16), width), F32),
            VMEM((owners * stations, width), BF16),
            pltpu.SemaphoreType.REGULAR, pltpu.SemaphoreType.REGULAR,
            dma((chunks, chips)), dma((chunks, chips)),
            dma((total_chunks, crossings)), dma((total_chunks, crossings)),
            dma((total_chunks + 1, major)), dma((total_chunks + 1, major)),
            dma((total_chunks + 1, major, sides)), dma((total_chunks + 1, major, sides)),
            dma((chunks, crossings)), dma((chunks, crossings)),
            dma((chunks, chips)), dma((chunks, chips)),
        ],
        compiler_params=pltpu.CompilerParams(
            collective_id=0, has_side_effects=True, vmem_limit_bytes=40 * 1024 * 1024
        ),
    )(sums, cells)

    rows = 512 if block_total % 512 == 0 else block_total
    return pl.pallas_call(
        functools.partial(anomaly_kernel, ranges, cell_dev, cell_pad, rows),
        in_specs=[whole] * 3,
        out_specs=[hbm] * 2,
        out_shape=[
            jax.ShapeDtypeStruct((block_total, days), F32),
            jax.ShapeDtypeStruct((cell_dev, 3 * days), F32),
        ],
        scratch_shapes=[
            VMEM((round_up(3 * stations, WINDOW) + WINDOW, 2 * days), BF16),
            VMEM((cell_dev, 3 * days), F32),
            VMEM((block_total, days), F32),
            dma((1,)), dma((block_total // rows,)),
        ],
        compiler_params=pltpu.CompilerParams(vmem_limit_bytes=40 * 1024 * 1024),
    )(masked, code, clim)


def solution(mesh):
    in_specs = (
        P(("sta", "yr"), None),
        P(None, ("sta", "yr")),
        P(("sta", "yr")),
        P("yr", "sta"),
        P("sta"),
    )
    out_specs = (P(("sta", "yr"), None), P("sta", None))

    def run(*args):
        return tuple(per_device(*args))

    return jax.shard_map(
        run, mesh=mesh, in_specs=in_specs, out_specs=out_specs, check_vma=False
    )
```
